512 devices in a mesh: member: 32 (over x, z), tile: 16 (over y, core).
Axes of the slice: x: 4, y: 8, z: 8, core: 2. Of those that a mesh axis runs over, the one named last changes fastest.
Arguments:
- ensemble: bfloat16 [256, 2048, 320], P('member', 'tile'), may hold values from -6 to 6
- departures: bfloat16 [2048, 128, 256], P(('tile', 'member')), may hold values from -6 to 6
- innovations: float32 [2048, 128], P(('tile', 'member')), may hold values from -12 to 12
- precision: float32 [2048, 128], P(('tile', 'member')), may hold values from 0.2 to 5
- obs_count: int32 [2048], P(('tile', 'member')), may hold values from 16 to 128
- tile_counts: int32 [16], replicated, may hold values from 0 to 128, as said below
Outputs:
- analysis: bfloat16 [256, 2048, 320], P('member', 'tile')
The draws below stay inside these ranges and needn't reach their ends.
Inputs may be any that keep to these rules, and one draw needn't show every extreme that they name: `tile_counts`: each count is a multiple of 32; all counts sum to 1024, and for every tile t the counts of tiles 0 to t - 1 sum to t * 32 * 2 plus or minus at most 32.
All inputs are finite; a program needn't handle non-finite values.
Results may differ from the reference program's by a relative error of at most 0.0049.
Values may be sent and summed in bfloat16 or wider, within the bound.
No kernel may reach another device: no remote copies, remote signals or barrier semaphores. Data moves between devices by JAX's collectives and lax.ppermute only.
A program may use at most 64 MiB of HBM per device.

```python
import math
import jax
import jax.numpy as jnp
from jax import lax

K = 256
V = 320
P_SIZE = 128
WORK = 2
ITERS = 6
LOC = 4
COLS = 2048
N_MEMBER = 32
N_TILE = 16


def draw_tile_counts(key, part):
    reach = WORK // 2
    walk_key, summit_key = jax.random.split(jax.random.fold_in(key, 11))
    offsets = jax.random.randint(walk_key, (N_TILE + 1,), -reach, reach + 1)
    borders = jnp.arange(N_TILE + 1)
    offsets = jnp.where((borders == 0) | (borders == N_TILE), 0, offsets)
    summit = jax.random.randint(summit_key, (), 1, N_TILE - 1)
    offsets = jnp.where(borders == summit, -reach, offsets)
    offsets = jnp.where(borders == summit + 1, reach, offsets)
    per_tile = WORK + offsets[1:] - offsets[:-1]
    return (per_tile * N_MEMBER).astype(jnp.int32)


def plant(drawn, own_key, low, high):
    dims = drawn.shape
    index_at = [jax.random.randint(jax.random.fold_in(own_key, axis), (), 0, dims[axis]) for axis in range(len(dims))]
    drawn = drawn.at[tuple(index_at)].set(low)
    longest = dims.index(max(dims))
    index_at[longest] = (index_at[longest] + 1) % dims[longest]
    return drawn.at[tuple(index_at)].set(high)


def levels(own_key, shape, cuts, least, top_value):
    level, own = 1.0, jax.random.fold_in(own_key, 6)
    for position, shards_of in cuts:
        steps = jnp.exp(jax.random.uniform(jax.random.fold_in(own, position), (shards_of,), jnp.float32, least / len(cuts), top_value / len(cuts)))
        level = level * jnp.repeat(steps, shape[position] // shards_of).reshape([-1 if axis == position else 1 for axis in range(len(shape))])
    return level


def gaussian(rng, shape, width, bound, cuts=(), held_as=jnp.bfloat16):
    factor_of = levels(rng, shape, cuts, -0.22, 0.18) if cuts else 1.0
    drawn = jax.random.normal(rng, shape, jnp.float32) * width * factor_of
    return jnp.minimum(jnp.maximum(drawn, -bound), bound).astype(held_as)


def setup_inputs(seed: int = 0) -> dict:
    streams_of = jax.random.split(jax.random.key(seed), 7)
    return {
        "ensemble": gaussian(streams_of[0], (K, COLS, V), 1.0, 6.0, ((0, 32), (1, 16))),
        "departures": gaussian(streams_of[1], (COLS, P_SIZE, K), 1.0, 6.0, ((0, 512),)),
        "innovations": gaussian(streams_of[2], (COLS, P_SIZE), 2.0, 12.0, ((0, 512),), jnp.float32),
        "precision": jnp.clip(jnp.exp(math.log(5.0) - 3.218876 * jax.random.uniform(streams_of[3], (COLS, P_SIZE), jnp.float32) ** levels(streams_of[3], (COLS, P_SIZE), ((0, 512),), -0.2, 0.2)), 0.2, 5.0),
        "obs_count": plant(jax.random.randint(streams_of[4], (COLS,), P_SIZE // 8, P_SIZE + 1), jax.random.fold_in(streams_of[4], 1), P_SIZE // 8, P_SIZE).astype(jnp.int32),
        "tile_counts": draw_tile_counts(jax.random.fold_in(streams_of[6], 71), 0),
    }


HIGHEST = lax.Precision.HIGHEST

def prepare(departures, innovations, precision, obs_count):
    row_ids = jnp.arange(departures.shape[1], dtype=jnp.int32)
    weight = jnp.where(row_ids[None, :] < obs_count[:, None], jnp.sqrt(precision), jnp.float32(0.0))
    scaled = (departures.astype(jnp.float32) * weight[:, :, None]).astype(jnp.bfloat16)
    signal = (weight * innovations).astype(jnp.bfloat16)
    return (scaled, signal)

def analyse(columns, scaled, signal):
    members = columns.shape[0]
    states = columns.astype(jnp.float32)
    average = lax.optimization_barrier(jnp.mean(states, axis=0))
    spread = (states - average[None]).astype(jnp.bfloat16)
    scaled_f = scaled.astype(jnp.float32)
    gram_matrix = jnp.einsum('npk,npj->nkj', scaled_f, scaled_f, precision=HIGHEST)
    pull_term = jnp.einsum('npk,np->nk', scaled_f, signal.astype(jnp.float32), precision=HIGHEST)
    identity = jnp.eye(members, dtype=jnp.float32)
    system = gram_matrix + (members - 1.0) * identity
    scale_norm = jnp.sqrt(lax.optimization_barrier(jnp.sum(system * system, axis=(1, 2))))
    root_iter = system / scale_norm[:, None, None]
    inverse_iter = jnp.broadcast_to(identity, system.shape)
    for repeat in range(ITERS):
        factor = 1.5 * identity - 0.5 * jnp.einsum('nij,njk->nik', inverse_iter, root_iter, precision=HIGHEST)
        if repeat + 1 < ITERS:
            root_iter = jnp.einsum('nij,njk->nik', root_iter, factor, precision=HIGHEST)
        inverse_iter = jnp.einsum('nij,njk->nik', factor, inverse_iter, precision=HIGHEST)
    halfway = jnp.einsum('njk,nk->nj', inverse_iter, pull_term, precision=HIGHEST)
    shift_w = jnp.einsum('njk,nk->nj', inverse_iter, halfway, precision=HIGHEST) / scale_norm[:, None]
    transform = (jnp.sqrt((members - 1.0) / scale_norm)[:, None, None] * inverse_iter + shift_w[:, :, None]).astype(jnp.bfloat16)
    update = jnp.einsum('njk,jnv->knv', transform.astype(jnp.float32), spread.astype(jnp.float32), precision=HIGHEST)
    return (average[None] + update).astype(jnp.bfloat16)

def reference(ensemble, departures, innovations, precision, obs_count, tile_counts):
    blocks = COLS // LOC
    states = ensemble.reshape(K, blocks, LOC, V).transpose(1, 0, 2, 3)

    def one_block(pieces):
        block_states, block_dep, block_inn, block_prec, block_count = pieces
        scaled, signal = prepare(block_dep, block_inn, block_prec, block_count)
        return analyse(block_states, scaled, signal)
    analysed = lax.map(one_block, (states, departures.reshape(blocks, LOC, P_SIZE, K), innovations.reshape(blocks, LOC, P_SIZE), precision.reshape(blocks, LOC, P_SIZE), obs_count.reshape(blocks, LOC)))
    analysed = analysed.transpose(1, 0, 2, 3).reshape(K, COLS, V)
    column_ids = jnp.arange(COLS, dtype=jnp.int32)
    tile_of = (column_ids // (N_MEMBER * LOC)).astype(jnp.int32)
    is_live = N_MEMBER * (column_ids % LOC) < jnp.take(tile_counts, tile_of)
    return jnp.where(is_live[None, :, None], analysed, ensemble)
```

```python
import jax
import jax.numpy as jnp
from jax import lax
from jax.experimental import pallas as pl
from jax.experimental.pallas import tpu as pltpu
from jax.sharding import PartitionSpec as P

ITERS = 6
F32 = jnp.float32
BF16 = jnp.bfloat16


def iota(shape, axis):
    return lax.broadcasted_iota(jnp.int32, shape, axis)


def dot(a, b, dims):
    return lax.dot_general(a, b, ((dims[:1], dims[1:]), ((), ())), preferred_element_type=F32)


def pack_kernel(x_ref, out_ref, rows_ref, *, slots, groups):
    part_rows, length, width = x_ref.shape
    capacity = width // groups
    head = (length // 128) * 128
    tail = length - head
    evens, odds = (slots + 1) // 2, slots // 2

    def pick(count, odd):
        shape = (count * groups, width)
        row = iota(shape, 0)
        slot = 2 * (row // groups) + odd
        return (iota(shape, 1) == (row % groups) * capacity + slot).astype(BF16)

    pick_even = pick(evens, 0)
    pick_odd = pick(odds, 1)
    low = iota((groups, 128), 1) < tail
    for m in range(part_rows):
        x = x_ref[m]
        even = dot(pick_even, jnp.concatenate([x, x[: 128 - tail]], axis=0), (1, 1))
        odd = dot(pick_odd, jnp.concatenate([x[head:], x], axis=0), (1, 1))
        here = pl.ds(m, groups, stride=part_rows)
        for p in range(evens):
            base = 2 * p * length
            a = even[p * groups : (p + 1) * groups]
            if p < odds:
                b = odd[p * groups : (p + 1) * groups]
                joined = jnp.concatenate(
                    [a[:, :head], jnp.where(low, a[:, head:], b[:, :128]), b[:, 128:]], axis=1
                )
                for t in range(2 * length // 128):
                    rows_ref[base // 128 + t, here, :] = joined[:, 128 * t : 128 * (t + 1)]
            else:
                for t in range(a.shape[1] // 128):
                    rows_ref[base // 128 + t, here, :] = a[:, 128 * t : 128 * (t + 1)]
    for t in range(rows_ref.shape[0]):
        end = min(128, out_ref.shape[1] - 128 * t)
        out_ref[:, pl.ds(128 * t, end)] = rows_ref[t][:, :end].astype(BF16)


def unpack_kernel(live_ref, x_ref, y_ref, out_ref, rows_ref, *, slots, groups):
    part_rows, length, width = x_ref.shape
    capacity = width // groups
    head = (length // 128) * 128
    tail = length - head
    evens, odds = (slots + 1) // 2, slots // 2

    def place(count, odd):
        shape = (count * groups, width)
        row = iota(shape, 0)
        slot = 2 * (row // groups) + odd
        return (iota(shape, 1) == (row % groups) * capacity + slot).astype(BF16)

    place_even = place(evens, 0)
    place_odd = place(odds, 1)
    for t in range(rows_ref.shape[0]):
        end = min(128, y_ref.shape[1] - 128 * t)
        rows_ref[t, :, pl.ds(0, end)] = y_ref[:, pl.ds(128 * t, end)].astype(F32)
    new = iota((length, width), 1) % capacity < live_ref[0]
    for m in range(part_rows):
        here = pl.ds(m, groups, stride=part_rows)
        parts = []
        for p in range(evens):
            first = 2 * p * length // 128
            tiles = [rows_ref[first + t, here, :] for t in range(head // 128 + 1)]
            parts.append(jnp.concatenate(tiles, axis=1)[:, :length])
        even = jnp.concatenate(parts, axis=0).astype(BF16)
        result = dot(even, place_even, (0, 0))
        parts = []
        for p in range(odds):
            first = (2 * p * length + head) // 128
            tiles = [rows_ref[first + t, here, :] for t in range(head // 128 + 1)]
            parts.append(jnp.concatenate(tiles, axis=1))
        odd = jnp.concatenate(parts, axis=0).astype(BF16)
        result = result + dot(odd, place_odd, (0, 0))[tail:]
        out_ref[m] = jnp.where(new, result, x_ref[m].astype(F32)).astype(BF16)


def split(x):
    high = x.astype(BF16)
    return high, (x - high.astype(F32)).astype(BF16)


def product(high, low, right_high, right_low):
    left = jnp.concatenate([high, low, high], axis=1)
    right = jnp.concatenate([right_high, right_high, right_low], axis=0)
    return dot(left, right, (1, 0))


def transform_kernel(
    live_ref, count_ref, dep_ref, inn_ref, prec_ref, out_ref, rest_ref, inner_ref, *, pair
):
    slots, members = out_ref.shape[0], out_ref.shape[1]
    obs = dep_ref.shape[1]
    rank = members - 1.0
    eye = (iota((members, members), 0) == iota((members, members), 1)).astype(F32)
    eye_obs = iota((obs, obs), 0) == iota((obs, obs), 1)

    def one_group(group, carry):
        base = group * pair
        f, z, norm_inv, pull = [], [], [], []
        for i in range(pair):
            slot = base + i
            live_row = iota((1, obs), 1) < count_ref[slot]
            weight = jnp.where(live_row, jnp.sqrt(prec_ref[pl.ds(slot, 1), :]), 0.0)
            column = jnp.sum(jnp.where(eye_obs, weight, 0.0), axis=1, keepdims=True)
            scaled = (dep_ref[slot].astype(F32) * column).astype(BF16)
            signal = (weight * inn_ref[pl.ds(slot, 1), :]).astype(BF16)
            gram = dot(scaled, scaled, (0, 0))
            pull.append(dot(jnp.broadcast_to(signal, (8, obs)), scaled, (1, 0))[:1])
            system = gram + rank * eye
            squares = jnp.sum(system * system, axis=0, keepdims=True)
            inv = 1.0 / jnp.sqrt(jnp.sum(squares, axis=1, keepdims=True))
            norm_inv.append(inv)
            f.append(1.5 - (0.5 * rank) * inv)
            z.append(f[i])
            rest = gram * (-0.5 * inv)
            rest_ref[i] = rest
            inner_ref[i] = rest

        def advance(i, f, square):
            rest = rest_ref[i]
            second = (2.0 * f) * rest + square
            right = split(rest)
            third = f * second + (f * f) * rest + product(*split(second), *right)
            rest_ref[i] = third - 1.5 * second
            return 1.5 - 1.5 * f * f + f * f * f

        for i in range(pair):
            both = split(rest_ref[i])
            f[i] = advance(i, f[i], product(*both, *both))

        def step(_, carried):
            f, z = list(carried[:pair]), list(carried[pair:])
            for i in range(pair):
                rest = rest_ref[i]
                inner = inner_ref[i]
                right = split(rest)
                left = split(inner)
                stack = [jnp.concatenate([a, b], axis=0) for a, b in zip(right, left)]
                both = product(*stack, *right)
                inner_ref[i] = f[i] * inner + z[i] * rest + both[members:]
                z[i] = f[i] * z[i]
                f[i] = advance(i, f[i], both[:members])
            return tuple(f) + tuple(z)

        carried = lax.fori_loop(0, ITERS - 2, step, tuple(f) + tuple(z))
        f, z = carried[:pair], carried[pair:]
        for i in range(pair):
            rest = rest_ref[i]
            inner = inner_ref[i]
            inner = f[i] * inner + z[i] * rest + product(*split(inner), *split(rest))
            whole = inner + (f[i] * z[i]) * eye
            halfway = jnp.sum(whole * pull[i], axis=1, keepdims=True)
            shift = jnp.sum(whole * halfway, axis=0, keepdims=True) * norm_inv[i]
            out_ref[base + i] = (jnp.sqrt(rank * norm_inv[i]) * whole + shift).astype(BF16)
        return carry

    busy = (jnp.clip(live_ref[0], 1, slots) + pair - 1) // pair

    def clear(group, carry):
        for i in range(pair):
            out_ref[group * pair + i] = jnp.zeros((members, members), BF16)
        return carry

    lax.fori_loop(0, busy, one_group, 0)
    lax.fori_loop(busy, slots // pair, clear, 0)


def apply_kernel(y_ref, t_ref, out_ref, *, slots, length):
    members = y_ref.shape[0]
    head = (length // 128) * 128
    tail = length - head
    low = iota((members, 128), 1) < tail
    for p in range((slots + 1) // 2):
        base = 2 * p * length
        size = 2 * length if 2 * p + 1 < slots else length
        here = pl.ds(base, size)
        states = y_ref[:, here].astype(F32)
        average = jnp.sum(states, axis=0, keepdims=True) * (1.0 / members)
        spread = (states - average).astype(BF16)
        if size == length:
            update = dot(t_ref[2 * p], spread, (1, 0))
        else:
            even = dot(t_ref[2 * p], spread[:, : head + 128], (1, 0))
            odd = dot(t_ref[2 * p + 1], spread[:, head:], (1, 0))
            update = jnp.concatenate(
                [even[:, :head], jnp.where(low, even[:, head:], odd[:, :128]), odd[:, 128:]], axis=1
            )
        out_ref[:, here] = (average + update).astype(BF16)


def exchange(blocks):
    return lax.all_to_all(blocks, "member", split_axis=0, concat_axis=0, tiled=True)


SMEM = pl.BlockSpec(memory_space=pltpu.SMEM)
VMEM = pl.BlockSpec(memory_space=pltpu.VMEM)
PARAMS = pltpu.CompilerParams(vmem_limit_bytes=48 * 2**20)


def lane_tiles(shape):
    return pltpu.VMEM((pl.cdiv(shape[1], 128), shape[0], 128), F32)


def pack(states, slots, groups):
    part_rows, length, _ = states.shape
    shape = (groups * part_rows, slots * length)
    return pl.pallas_call(
        lambda *refs: pack_kernel(*refs, slots=slots, groups=groups),
        out_shape=jax.ShapeDtypeStruct(shape, BF16),
        in_specs=[VMEM],
        out_specs=VMEM,
        scratch_shapes=[lane_tiles(shape)],
        compiler_params=PARAMS,
        name="pack",
    )(states)


def unpack(live, states, finished, slots, groups):
    return pl.pallas_call(
        lambda *refs: unpack_kernel(*refs, slots=slots, groups=groups),
        out_shape=jax.ShapeDtypeStruct(states.shape, BF16),
        in_specs=[SMEM, VMEM, VMEM],
        out_specs=VMEM,
        scratch_shapes=[lane_tiles(finished.shape)],
        compiler_params=PARAMS,
        name="unpack",
    )(live, states, finished)


def transforms(live, departures, innovations, precision, obs_count, slots):
    members = departures.shape[2]
    pair = 2
    whole = (members, members)
    return pl.pallas_call(
        lambda *refs: transform_kernel(*refs, pair=pair),
        out_shape=jax.ShapeDtypeStruct((slots + slots % pair, *whole), BF16),
        in_specs=[SMEM, SMEM, VMEM, VMEM, VMEM],
        out_specs=VMEM,
        scratch_shapes=[pltpu.VMEM((pair, *whole), F32), pltpu.VMEM((pair, *whole), F32)],
        compiler_params=PARAMS,
        name="transform",
    )(live, obs_count, departures, innovations, precision)


def apply(states, transform, slots, length):
    return pl.pallas_call(
        lambda *refs: apply_kernel(*refs, slots=slots, length=length),
        out_shape=jax.ShapeDtypeStruct(states.shape, BF16),
        in_specs=[VMEM, VMEM],
        out_specs=VMEM,
        compiler_params=PARAMS,
        name="apply",
    )(states, transform)


def analyse(slots, groups, live, states, departures, innovations, precision, obs_count):
    part_rows, length, _ = states.shape
    members = groups * part_rows
    width = slots * length
    packed = pack(states, slots, groups)
    columns = exchange(packed.reshape(groups, part_rows, width)).reshape(members, width)
    transform = transforms(live, departures, innovations, precision, obs_count, slots)
    result = apply(columns, transform, slots, length)
    home = exchange(result.reshape(groups, part_rows, width)).reshape(members, width)
    return unpack(live, states, home, slots, groups)


def on_device(ensemble, departures, innovations, precision, obs_count, tile_counts):
    groups = lax.axis_size("member")
    capacity = departures.shape[0]
    here = jnp.arange(tile_counts.shape[0]) == lax.axis_index("tile")
    live = (jnp.sum(jnp.where(here, tile_counts, 0), keepdims=True) // groups).astype(jnp.int32)
    states = ensemble.transpose(0, 2, 1)
    result = analyse(
        capacity, groups, live, states, departures, innovations, precision, obs_count
    )
    return result.transpose(0, 2, 1)


def solution(mesh):
    placed = (
        P("member", "tile", None),
        P(("tile", "member"), None, None),
        P(("tile", "member"), None),
        P(("tile", "member"), None),
        P(("tile", "member")),
        P(),
    )
    return jax.shard_map(
        on_device, mesh=mesh, in_specs=placed, out_specs=P("member", "tile", None), check_vma=False
    )
```

```python
import jax
import jax.numpy as jnp
from jax import lax
from jax.experimental import pallas as pl
from jax.experimental.pallas import tpu as pltpu
from jax.sharding import PartitionSpec as P

ITERS = 6
F32 = jnp.float32
BF16 = jnp.bfloat16


def iota(shape, axis):
    return lax.broadcasted_iota(jnp.int32, shape, axis)


def dot(a, b, dims):
    return lax.dot_general(a, b, ((dims[:1], dims[1:]), ((), ())), preferred_element_type=F32)


def pack_kernel(x_ref, out_ref, rows_ref, *, slots, groups):
    part_rows, length, width = x_ref.shape
    capacity = width // groups
    head = (length // 128) * 128
    tail = length - head
    evens, odds = (slots + 1) // 2, slots // 2

    def pick(count, odd):
        shape = (count * groups, width)
        row = iota(shape, 0)
        slot = 2 * (row // groups) + odd
        return (iota(shape, 1) == (row % groups) * capacity + slot).astype(BF16)

    pick_even = pick(evens, 0)
    pick_odd = pick(odds, 1)
    low = iota((groups, 128), 1) < tail
    for m in range(part_rows):
        x = x_ref[m]
        even = dot(pick_even, jnp.concatenate([x, x[: 128 - tail]], axis=0), (1, 1))
        odd = dot(pick_odd, jnp.concatenate([x[head:], x], axis=0), (1, 1))
        here = pl.ds(m, groups, stride=part_rows)
        for p in range(evens):
            base = 2 * p * length
            a = even[p * groups : (p + 1) * groups]
            if p < odds:
                b = odd[p * groups : (p + 1) * groups]
                joined = jnp.concatenate(
                    [a[:, :head], jnp.where(low, a[:, head:], b[:, :128]), b[:, 128:]], axis=1
                )
                for t in range(2 * length // 128):
                    rows_ref[base // 128 + t, here, :] = joined[:, 128 * t : 128 * (t + 1)]
            else:
                for t in range(a.shape[1] // 128):
                    rows_ref[base // 128 + t, here, :] = a[:, 128 * t : 128 * (t + 1)]
    for t in range(rows_ref.shape[0]):
        end = min(128, out_ref.shape[1] - 128 * t)
        out_ref[:, pl.ds(128 * t, end)] = rows_ref[t][:, :end].astype(BF16)


def unpack_kernel(live_ref, x_ref, y_ref, out_ref, rows_ref, *, slots, groups):
    part_rows, length, width = x_ref.shape
    capacity = width // groups
    head = (length // 128) * 128
    tail = length - head
    evens, odds = (slots + 1) // 2, slots // 2

    def place(count, odd):
        shape = (count * groups, width)
        row = iota(shape, 0)
        slot = 2 * (row // groups) + odd
        return (iota(shape, 1) == (row % groups) * capacity + slot).astype(BF16)

    place_even = place(evens, 0)
    place_odd = place(odds, 1)
    for t in range(rows_ref.shape[0]):
        end = min(128, y_ref.shape[1] - 128 * t)
        rows_ref[t, :, pl.ds(0, end)] = y_ref[:, pl.ds(128 * t, end)].astype(F32)
    new = iota((length, width), 1) % capacity < live_ref[0]
    for m in range(part_rows):
        here = pl.ds(m, groups, stride=part_rows)
        parts = []
        for p in range(evens):
            first = 2 * p * length // 128
            tiles = [rows_ref[first + t, here, :] for t in range(head // 128 + 1)]
            parts.append(jnp.concatenate(tiles, axis=1)[:, :length])
        even = jnp.concatenate(parts, axis=0).astype(BF16)
        result = dot(even, place_even, (0, 0))
        parts = []
        for p in range(odds):
            first = (2 * p * length + head) // 128
            tiles = [rows_ref[first + t, here, :] for t in range(head // 128 + 1)]
            parts.append(jnp.concatenate(tiles, axis=1))
        odd = jnp.concatenate(parts, axis=0).astype(BF16)
        result = result + dot(odd, place_odd, (0, 0))[tail:]
        out_ref[m] = jnp.where(new, result, x_ref[m].astype(F32)).astype(BF16)


def split(x):
    high = x.astype(BF16)
    return high, (x - high.astype(F32)).astype(BF16)


def left_of(x):
    high, low = split(x)
    return jnp.concatenate([high, low, high, low], axis=1)


def right_of(x):
    high, low = split(x)
    return jnp.concatenate([high, high, low, low], axis=0)


def total(x):
    return jnp.sum(jnp.sum(x, axis=0, keepdims=True), axis=1, keepdims=True)


def transform_kernel(
    count_ref, dep_ref, inn_ref, prec_ref, out_ref, scaled_ref, h_ref, right_ref, rest_ref, inner_ref
):
    slots, members = out_ref.shape[0], out_ref.shape[1]
    obs = dep_ref.shape[1]
    rank = members - 1.0
    eye = (iota((members, members), 0) == iota((members, members), 1)).astype(F32)
    on_diagonal = iota((obs, obs), 0) == iota((obs, obs), 1)
    eye_obs = on_diagonal.astype(F32)
    f, z, norm_inv, signal = [], [], [], []
    for i in range(slots):
        weight = jnp.where(iota((1, obs), 1) < count_ref[i], jnp.sqrt(prec_ref[i : i + 1, :]), 0.0)
        column = jnp.sum(jnp.where(on_diagonal, weight, 0.0), axis=1, keepdims=True)
        scaled = (dep_ref[i].astype(F32) * column).astype(BF16)
        scaled_ref[i] = scaled
        signal.append((weight * inn_ref[i : i + 1, :]).astype(BF16).astype(F32))
        outer = dot(scaled, scaled, (1, 1))
        squares = total(outer * outer) + (2.0 * rank) * total(outer * eye_obs)
        norm_inv.append(1.0 / jnp.sqrt(squares + members * rank * rank))
        f.append(1.5 - (0.5 * rank) * norm_inv[i])
        z.append(f[i])
        h_ref[i] = outer * norm_inv[i]
    for i in range(slots):
        h = h_ref[i]
        right = right_of(h)
        right_ref[i] = right
        second = 0.25 * h - f[i] * eye_obs
        third = (f[i] * second + (0.5 * f[i]) * h - (0.5 * f[i] * f[i]) * eye_obs) - 0.125 * dot(
            left_of(h), right, (1, 0)
        )
        rest_ref[i] = third - 1.5 * second
        inner_ref[i] = -0.5 * eye_obs
        f[i] = 1.5 - 1.5 * f[i] * f[i] + f[i] * f[i] * f[i]

    def step(_, carried):
        f, z = list(carried[:slots]), list(carried[slots:])
        moved = [left_of(dot(left_of(rest_ref[i]), right_ref[i], (1, 0))) for i in range(slots)]
        seconds = []
        for i in range(slots):
            rest, inner = rest_ref[i], inner_ref[i]
            both = dot(moved[i], right_of(jnp.concatenate([inner, rest], axis=1)), (1, 0))
            inner_ref[i] = f[i] * inner + z[i] * rest + both[:, :obs]
            seconds.append((2.0 * f[i]) * rest + both[:, obs:])
            z[i] = f[i] * z[i]
        for i in range(slots):
            third = dot(moved[i], right_of(seconds[i]), (1, 0))
            third = third + f[i] * seconds[i] + (f[i] * f[i]) * rest_ref[i]
            rest_ref[i] = third - 1.5 * seconds[i]
            f[i] = 1.5 - 1.5 * f[i] * f[i] + f[i] * f[i] * f[i]
        return tuple(f) + tuple(z)

    carried = lax.fori_loop(0, ITERS - 2, step, tuple(f) + tuple(z))
    f, z = carried[:slots], carried[slots:]
    for i in range(slots):
        rest, inner = rest_ref[i], inner_ref[i]
        moved = left_of(dot(left_of(rest), right_ref[i], (1, 0)))
        inner_ref[i] = f[i] * inner + z[i] * rest + dot(moved, right_of(inner), (1, 0))
    for i in range(slots):
        inner, h, scaled = inner_ref[i], h_ref[i], scaled_ref[i]
        scale = f[i] * z[i]
        pull = signal[i]
        for _ in range(2):
            across = jnp.sum(inner * pull, axis=1, keepdims=True)
            pull = scale * pull + jnp.sum(h * across, axis=0, keepdims=True)
        pieces = []
        for _ in range(3):
            pieces.append(pull.astype(BF16).astype(F32))
            pull = pull - pieces[-1]
        pieces.append(jnp.zeros((5, obs), F32))
        rows = dot(jnp.concatenate(pieces, axis=0).astype(BF16), scaled, (1, 0))
        shift = jnp.sum(rows, axis=0, keepdims=True) * norm_inv[i]
        twice = jnp.concatenate([scaled, scaled], axis=0)
        spanned = dot(jnp.concatenate(split(inner), axis=1), twice, (1, 0))
        spanned = dot(twice, jnp.concatenate(split(spanned), axis=0), (0, 0))
        gain = jnp.sqrt(rank * norm_inv[i])
        out_ref[i] = (gain * (scale * eye + norm_inv[i] * spanned) + shift).astype(BF16)


def apply_kernel(y_ref, t_ref, out_ref, *, slots, length):
    members = y_ref.shape[0]
    head = (length // 128) * 128
    tail = length - head
    low = iota((members, 128), 1) < tail
    for p in range((slots + 1) // 2):
        base = 2 * p * length
        size = 2 * length if 2 * p + 1 < slots else length
        here = pl.ds(base, size)
        states = y_ref[:, here].astype(F32)
        average = jnp.sum(states, axis=0, keepdims=True) * (1.0 / members)
        spread = (states - average).astype(BF16)
        if size == length:
            update = dot(t_ref[2 * p], spread, (1, 0))
        else:
            even = dot(t_ref[2 * p], spread[:, : head + 128], (1, 0))
            odd = dot(t_ref[2 * p + 1], spread[:, head:], (1, 0))
            update = jnp.concatenate(
                [even[:, :head], jnp.where(low, even[:, head:], odd[:, :128]), odd[:, 128:]], axis=1
            )
        out_ref[:, here] = (average + update).astype(BF16)


def exchange(blocks):
    return lax.all_to_all(blocks, "member", split_axis=0, concat_axis=0, tiled=True)


SMEM = pl.BlockSpec(memory_space=pltpu.SMEM)
VMEM = pl.BlockSpec(memory_space=pltpu.VMEM)
PARAMS = pltpu.CompilerParams(vmem_limit_bytes=48 * 2**20)


def lane_tiles(shape):
    return pltpu.VMEM((pl.cdiv(shape[1], 128), shape[0], 128), F32)


def pack(states, slots, groups):
    part_rows, length, _ = states.shape
    shape = (groups * part_rows, slots * length)
    return pl.pallas_call(
        lambda *refs: pack_kernel(*refs, slots=slots, groups=groups),
        out_shape=jax.ShapeDtypeStruct(shape, BF16),
        in_specs=[VMEM],
        out_specs=VMEM,
        scratch_shapes=[lane_tiles(shape)],
        compiler_params=PARAMS,
        name="pack",
    )(states)


def unpack(live, states, finished, slots, groups):
    return pl.pallas_call(
        lambda *refs: unpack_kernel(*refs, slots=slots, groups=groups),
        out_shape=jax.ShapeDtypeStruct(states.shape, BF16),
        in_specs=[SMEM, VMEM, VMEM],
        out_specs=VMEM,
        scratch_shapes=[lane_tiles(finished.shape)],
        compiler_params=PARAMS,
        name="unpack",
    )(live, states, finished)


def transforms(departures, innovations, precision, obs_count, slots):
    _, obs, members = departures.shape
    square = pltpu.VMEM((slots, obs, obs), F32)
    return pl.pallas_call(
        transform_kernel,
        out_shape=jax.ShapeDtypeStruct((slots, members, members), BF16),
        in_specs=[SMEM, VMEM, VMEM, VMEM],
        out_specs=VMEM,
        scratch_shapes=[
            pltpu.VMEM((slots, obs, members), BF16),
            square,
            pltpu.VMEM((slots, 4 * obs, obs), BF16),
            square,
            square,
        ],
        compiler_params=PARAMS,
        name="transform",
    )(obs_count, departures, innovations, precision)


def apply(states, transform, slots, length):
    return pl.pallas_call(
        lambda *refs: apply_kernel(*refs, slots=slots, length=length),
        out_shape=jax.ShapeDtypeStruct(states.shape, BF16),
        in_specs=[VMEM, VMEM],
        out_specs=VMEM,
        compiler_params=PARAMS,
        name="apply",
    )(states, transform)


def analyse(slots, groups, live, states, departures, innovations, precision, obs_count):
    part_rows, length, _ = states.shape
    members = groups * part_rows
    width = slots * length
    packed = pack(states, slots, groups)
    columns = exchange(packed.reshape(groups, part_rows, width)).reshape(members, width)
    transform = transforms(departures, innovations, precision, obs_count, slots)
    result = apply(columns, transform, slots, length)
    home = exchange(result.reshape(groups, part_rows, width)).reshape(members, width)
    return unpack(live, states, home, slots, groups)


def on_device(ensemble, departures, innovations, precision, obs_count, tile_counts):
    groups = lax.axis_size("member")
    capacity = departures.shape[0]
    here = jnp.arange(tile_counts.shape[0]) == lax.axis_index("tile")
    live = (jnp.sum(jnp.where(here, tile_counts, 0), keepdims=True) // groups).astype(jnp.int32)
    states = ensemble.transpose(0, 2, 1)
    result = analyse(
        capacity, groups, live, states, departures, innovations, precision, obs_count
    )
    return result.transpose(0, 2, 1)


def solution(mesh):
    placed = (
        P("member", "tile", None),
        P(("tile", "member"), None, None),
        P(("tile", "member"), None),
        P(("tile", "member"), None),
        P(("tile", "member")),
        P(),
    )
    return jax.shard_map(
        on_device, mesh=mesh, in_specs=placed, out_specs=P("member", "tile", None), check_vma=False
    )
```

```python
import jax
import jax.numpy as jnp
from jax import lax
from jax.experimental import pallas as pl
from jax.experimental.pallas import tpu as pltpu
from jax.sharding import PartitionSpec as P

ITERS = 6
F32 = jnp.float32
BF16 = jnp.bfloat16


def iota(shape, axis):
    return lax.broadcasted_iota(jnp.int32, shape, axis)


def dot(a, b, dims):
    return lax.dot_general(a, b, ((dims[:1], dims[1:]), ((), ())), preferred_element_type=F32)


def pack_kernel(x_ref, out_ref, rows_ref, *, slots, groups):
    part_rows, length, width = x_ref.shape
    capacity = width // groups
    head = (length // 128) * 128
    tail = length - head
    evens, odds = (slots + 1) // 2, slots // 2

    def pick(count, odd):
        shape = (count * groups, width)
        row = iota(shape, 0)
        slot = 2 * (row // groups) + odd
        return (iota(shape, 1) == (row % groups) * capacity + slot).astype(BF16)

    pick_even = pick(evens, 0)
    pick_odd = pick(odds, 1)
    low = iota((groups, 128), 1) < tail
    for m in range(part_rows):
        x = x_ref[m]
        even = dot(pick_even, jnp.concatenate([x, x[: 128 - tail]], axis=0), (1, 1))
        odd = dot(pick_odd, jnp.concatenate([x[head:], x], axis=0), (1, 1))
        here = pl.ds(m, groups, stride=part_rows)
        for p in range(evens):
            base = 2 * p * length
            a = even[p * groups : (p + 1) * groups]
            if p < odds:
                b = odd[p * groups : (p + 1) * groups]
                joined = jnp.concatenate(
                    [a[:, :head], jnp.where(low, a[:, head:], b[:, :128]), b[:, 128:]], axis=1
                )
                for t in range(2 * length // 128):
                    rows_ref[base // 128 + t, here, :] = joined[:, 128 * t : 128 * (t + 1)]
            else:
                for t in range(a.shape[1] // 128):
                    rows_ref[base // 128 + t, here, :] = a[:, 128 * t : 128 * (t + 1)]
    for t in range(rows_ref.shape[0]):
        end = min(128, out_ref.shape[1] - 128 * t)
        out_ref[:, pl.ds(128 * t, end)] = rows_ref[t][:, :end].astype(BF16)


def unpack_kernel(live_ref, x_ref, y_ref, out_ref, rows_ref, *, slots, groups):
    part_rows, length, width = x_ref.shape
    capacity = width // groups
    head = (length // 128) * 128
    tail = length - head
    evens, odds = (slots + 1) // 2, slots // 2

    def place(count, odd):
        shape = (count * groups, width)
        row = iota(shape, 0)
        slot = 2 * (row // groups) + odd
        return (iota(shape, 1) == (row % groups) * capacity + slot).astype(BF16)

    place_even = place(evens, 0)
    place_odd = place(odds, 1)
    for t in range(rows_ref.shape[0]):
        end = min(128, y_ref.shape[1] - 128 * t)
        rows_ref[t, :, pl.ds(0, end)] = y_ref[:, pl.ds(128 * t, end)].astype(F32)
    new = iota((length, width), 1) % capacity < live_ref[0]
    for m in range(part_rows):
        here = pl.ds(m, groups, stride=part_rows)
        parts = []
        for p in range(evens):
            first = 2 * p * length // 128
            tiles = [rows_ref[first + t, here, :] for t in range(head // 128 + 1)]
            parts.append(jnp.concatenate(tiles, axis=1)[:, :length])
        even = jnp.concatenate(parts, axis=0).astype(BF16)
        result = dot(even, place_even, (0, 0))
        parts = []
        for p in range(odds):
            first = (2 * p * length + head) // 128
            tiles = [rows_ref[first + t, here, :] for t in range(head // 128 + 1)]
            parts.append(jnp.concatenate(tiles, axis=1))
        odd = jnp.concatenate(parts, axis=0).astype(BF16)
        result = result + dot(odd, place_odd, (0, 0))[tail:]
        out_ref[m] = jnp.where(new, result, x_ref[m].astype(F32)).astype(BF16)


def split(x):
    high = x.astype(BF16)
    return high, (x - high.astype(F32)).astype(BF16)


def left_of(x):
    high, low = split(x)
    return jnp.concatenate([high, low, high, low], axis=1)


def right_of(x):
    high, low = split(x)
    return jnp.concatenate([high, high, low, low], axis=0)


def total(x):
    return jnp.sum(jnp.sum(x, axis=0, keepdims=True), axis=1, keepdims=True)


def transform_kernel(
    count_ref, dep_ref, inn_ref, prec_ref, out_ref, scaled_ref, h_ref, right_ref, rest_ref, inner_ref
):
    slots, members = out_ref.shape[0], out_ref.shape[1]
    obs = dep_ref.shape[1]
    rank = members - 1.0
    eye = (iota((members, members), 0) == iota((members, members), 1)).astype(F32)
    on_diagonal = iota((obs, obs), 0) == iota((obs, obs), 1)
    eye_obs = on_diagonal.astype(F32)
    f, z, norm_inv, signal = [], [], [], []
    for i in range(slots):
        weight = jnp.where(iota((1, obs), 1) < count_ref[i], jnp.sqrt(prec_ref[i : i + 1, :]), 0.0)
        column = jnp.sum(jnp.where(on_diagonal, weight, 0.0), axis=1, keepdims=True)
        scaled = (dep_ref[i].astype(F32) * column).astype(BF16)
        scaled_ref[i] = scaled
        signal.append((weight * inn_ref[i : i + 1, :]).astype(BF16).astype(F32))
        outer = dot(scaled, scaled, (1, 1))
        squares = total(outer * outer) + (2.0 * rank) * total(outer * eye_obs)
        norm_inv.append(1.0 / jnp.sqrt(squares + members * rank * rank))
        f.append(1.5 - (0.5 * rank) * norm_inv[i])
        z.append(f[i])
        h_ref[i] = outer * norm_inv[i]
    for i in range(slots):
        h = h_ref[i]
        right = right_of(h)
        right_ref[i] = right
        second = 0.25 * h - f[i] * eye_obs
        third = (f[i] * second + (0.5 * f[i]) * h - (0.5 * f[i] * f[i]) * eye_obs) - 0.125 * dot(
            left_of(h), right, (1, 0)
        )
        rest_ref[i] = third - 1.5 * second
        inner_ref[i] = -0.5 * eye_obs
        f[i] = 1.5 - 1.5 * f[i] * f[i] + f[i] * f[i] * f[i]

    def step(_, carried):
        f, z = list(carried[:slots]), list(carried[slots:])
        moved = [left_of(dot(left_of(rest_ref[i]), right_ref[i], (1, 0))) for i in range(slots)]
        seconds = []
        for i in range(slots):
            rest, inner = rest_ref[i], inner_ref[i]
            both = dot(moved[i], right_of(jnp.concatenate([inner, rest], axis=1)), (1, 0))
            inner_ref[i] = f[i] * inner + z[i] * rest + both[:, :obs]
            seconds.append((2.0 * f[i]) * rest + both[:, obs:])
            z[i] = f[i] * z[i]
        for i in range(slots):
            third = dot(moved[i], right_of(seconds[i]), (1, 0))
            third = third + f[i] * seconds[i] + (f[i] * f[i]) * rest_ref[i]
            rest_ref[i] = third - 1.5 * seconds[i]
            f[i] = 1.5 - 1.5 * f[i] * f[i] + f[i] * f[i] * f[i]
        return tuple(f) + tuple(z)

    carried = lax.fori_loop(0, ITERS - 2, step, tuple(f) + tuple(z))
    f, z = carried[:slots], carried[slots:]
    for i in range(slots):
        rest, inner = rest_ref[i], inner_ref[i]
        moved = left_of(dot(left_of(rest), right_ref[i], (1, 0)))
        inner_ref[i] = f[i] * inner + z[i] * rest + dot(moved, right_of(inner), (1, 0))
    for i in range(slots):
        inner, h, scaled = inner_ref[i], h_ref[i], scaled_ref[i]
        scale = f[i] * z[i]
        pull = signal[i]
        for _ in range(2):
            across = jnp.sum(inner * pull, axis=1, keepdims=True)
            pull = scale * pull + jnp.sum(h * across, axis=0, keepdims=True)
        pieces = []
        for _ in range(3):
            pieces.append(pull.astype(BF16).astype(F32))
            pull = pull - pieces[-1]
        pieces.append(jnp.zeros((5, obs), F32))
        rows = dot(jnp.concatenate(pieces, axis=0).astype(BF16), scaled, (1, 0))
        shift = jnp.sum(rows, axis=0, keepdims=True) * norm_inv[i]
        twice = jnp.concatenate([scaled, scaled], axis=0)
        spanned = dot(jnp.concatenate(split(inner), axis=1), twice, (1, 0))
        spanned = dot(twice, jnp.concatenate(split(spanned), axis=0), (0, 0))
        gain = jnp.sqrt(rank * norm_inv[i])
        out_ref[i] = (gain * (scale * eye + norm_inv[i] * spanned) + shift).astype(BF16)


def apply_kernel(y_ref, t_ref, out_ref, *, slots, length):
    members = y_ref.shape[0]
    head = (length // 128) * 128
    tail = length - head
    low = iota((members, 128), 1) < tail
    for p in range((slots + 1) // 2):
        base = 2 * p * length
        size = 2 * length if 2 * p + 1 < slots else length
        here = pl.ds(base, size)
        states = y_ref[:, here].astype(F32)
        average = jnp.sum(states, axis=0, keepdims=True) * (1.0 / members)
        spread = (states - average).astype(BF16)
        if size == length:
            update = dot(t_ref[2 * p], spread, (1, 0))
        else:
            even = dot(t_ref[2 * p], spread[:, : head + 128], (1, 0))
            odd = dot(t_ref[2 * p + 1], spread[:, head:], (1, 0))
            update = jnp.concatenate(
                [even[:, :head], jnp.where(low, even[:, head:], odd[:, :128]), odd[:, 128:]], axis=1
            )
        out_ref[:, here] = (average + update).astype(BF16)


def exchange(blocks):
    return lax.all_to_all(blocks, "member", split_axis=0, concat_axis=0, tiled=True)


SMEM = pl.BlockSpec(memory_space=pltpu.SMEM)
VMEM = pl.BlockSpec(memory_space=pltpu.VMEM)
PARAMS = pltpu.CompilerParams(vmem_limit_bytes=48 * 2**20)


def lane_tiles(shape):
    return pltpu.VMEM((pl.cdiv(shape[1], 128), shape[0], 128), F32)


def pack(states, slots, groups):
    part_rows, length, _ = states.shape
    shape = (groups * part_rows, slots * length)
    return pl.pallas_call(
        lambda *refs: pack_kernel(*refs, slots=slots, groups=groups),
        out_shape=jax.ShapeDtypeStruct(shape, BF16),
        in_specs=[VMEM],
        out_specs=VMEM,
        scratch_shapes=[lane_tiles(shape)],
        compiler_params=PARAMS,
        name="pack",
    )(states)


def unpack(live, states, finished, slots, groups):
    return pl.pallas_call(
        lambda *refs: unpack_kernel(*refs, slots=slots, groups=groups),
        out_shape=jax.ShapeDtypeStruct(states.shape, BF16),
        in_specs=[SMEM, VMEM, VMEM],
        out_specs=VMEM,
        scratch_shapes=[lane_tiles(finished.shape)],
        compiler_params=PARAMS,
        name="unpack",
    )(live, states, finished)


def transforms(departures, innovations, precision, obs_count, slots):
    _, obs, members = departures.shape
    square = pltpu.VMEM((slots, obs, obs), F32)
    return pl.pallas_call(
        transform_kernel,
        out_shape=jax.ShapeDtypeStruct((slots, members, members), BF16),
        in_specs=[SMEM, VMEM, VMEM, VMEM],
        out_specs=VMEM,
        scratch_shapes=[
            pltpu.VMEM((slots, obs, members), BF16),
            square,
            pltpu.VMEM((slots, 4 * obs, obs), BF16),
            square,
            square,
        ],
        compiler_params=PARAMS,
        name="transform",
    )(obs_count, departures, innovations, precision)


def apply(states, transform, slots, length):
    return pl.pallas_call(
        lambda *refs: apply_kernel(*refs, slots=slots, length=length),
        out_shape=jax.ShapeDtypeStruct(states.shape, BF16),
        in_specs=[VMEM, VMEM],
        out_specs=VMEM,
        compiler_params=PARAMS,
        name="apply",
    )(states, transform)


def with_slots(slots, groups):
    def run(live, states, packed, departures, innovations, precision, obs_count):
        part_rows, length, _ = states.shape
        members = groups * part_rows
        width = slots * length
        sent = packed[:, :width].reshape(groups, part_rows, width)
        columns = exchange(sent).reshape(members, width)
        transform = transforms(departures, innovations, precision, obs_count, slots)
        result = apply(columns, transform, slots, length)
        home = exchange(result.reshape(groups, part_rows, width)).reshape(members, width)
        return unpack(live, states, home, slots, groups)

    return run


def on_device(ensemble, departures, innovations, precision, obs_count, tile_counts):
    groups = lax.axis_size("member")
    capacity = departures.shape[0]
    here = jnp.arange(tile_counts.shape[0]) == lax.axis_index("tile")
    live = (jnp.sum(jnp.where(here, tile_counts, 0), keepdims=True) // groups).astype(jnp.int32)
    states = ensemble.transpose(0, 2, 1)
    packed = pack(states, capacity, groups)
    fewest = 2
    result = lax.switch(
        jnp.clip(live[0], fewest, capacity) - fewest,
        [with_slots(slots, groups) for slots in range(fewest, capacity + 1)],
        live,
        states,
        packed,
        departures,
        innovations,
        precision,
        obs_count,
    )
    return result.transpose(0, 2, 1)


def solution(mesh):
    placed = (
        P("member", "tile", None),
        P(("tile", "member"), None, None),
        P(("tile", "member"), None),
        P(("tile", "member"), None),
        P(("tile", "member")),
        P(),
    )
    return jax.shard_map(
        on_device, mesh=mesh, in_specs=placed, out_specs=P("member", "tile", None), check_vma=False
    )
```

```python
import jax
import jax.numpy as jnp
from jax import lax
from jax.experimental import pallas as pl
from jax.experimental.pallas import tpu as pltpu
from jax.sharding import PartitionSpec as P

ITERS = 6
F32 = jnp.float32
BF16 = jnp.bfloat16


def iota(shape, axis):
    return lax.broadcasted_iota(jnp.int32, shape, axis)


def dot(a, b, dims):
    return lax.dot_general(a, b, ((dims[:1], dims[1:]), ((), ())), preferred_element_type=F32)


def pack_kernel(counts_ref, x_ref, *refs, chunks, groups, fewest):
    out_refs, index_ref, live_ref, rows_ref = refs[:-3], refs[-3], refs[-2], refs[-1]
    part_rows, length, width = x_ref.shape
    capacity = width // groups
    head = (length // 128) * 128
    tail = length - head
    live = counts_ref[lax.axis_index("tile")] // groups
    live_ref[0] = live
    index_ref[0] = jnp.clip(live, fewest, capacity) - fewest

    def pick(odd):
        shape = (capacity // 2 * groups, width)
        row = iota(shape, 0)
        slot = 2 * (row // groups) + odd
        return (iota(shape, 1) == (row % groups) * capacity + slot).astype(BF16)

    pick_even = pick(0)
    pick_odd = pick(1)
    low = iota((groups, 128), 1) < tail
    for m in range(part_rows):
        x = x_ref[m]
        even = dot(pick_even, jnp.concatenate([x, x[: 128 - tail]], axis=0), (1, 1))
        odd = dot(pick_odd, jnp.concatenate([x[head:], x], axis=0), (1, 1))
        here = pl.ds(m, groups, stride=part_rows)
        for p in range(capacity // 2):
            base = 2 * p * length // 128
            a = even[p * groups : (p + 1) * groups]
            b = odd[p * groups : (p + 1) * groups]
            joined = jnp.concatenate(
                [a[:, :head], jnp.where(low, a[:, head:], b[:, :128]), b[:, 128:]], axis=1
            )
            for t in range(2 * length // 128):
                rows_ref[base + t, here, :] = joined[:, 128 * t : 128 * (t + 1)]
    for (start, size), out_ref in zip(chunks, out_refs):
        for t in range(pl.cdiv(size * length, 128)):
            end = min(128, size * length - 128 * t)
            tile = rows_ref[start * length // 128 + t]
            out_ref[:, pl.ds(128 * t, end)] = tile[:, :end].astype(BF16)


def unpack_kernel(live_ref, x_ref, *refs, slots, groups):
    y_refs, out_ref, rows_ref = refs[:-2], refs[-2], refs[-1]
    part_rows, length, width = x_ref.shape
    capacity = width // groups
    head = (length // 128) * 128
    tail = length - head
    evens, odds = (slots + 1) // 2, slots // 2

    def place(count, odd):
        shape = (count * groups, width)
        row = iota(shape, 0)
        slot = 2 * (row // groups) + odd
        return (iota(shape, 1) == (row % groups) * capacity + slot).astype(BF16)

    place_even = place(evens, 0)
    place_odd = place(odds, 1)
    base = 0
    for y_ref in y_refs:
        for t in range(pl.cdiv(y_ref.shape[1], 128)):
            end = min(128, y_ref.shape[1] - 128 * t)
            rows_ref[base, :, pl.ds(0, end)] = y_ref[:, pl.ds(128 * t, end)].astype(F32)
            base += 1
    new = iota((length, width), 1) % capacity < live_ref[0]
    for m in range(part_rows):
        here = pl.ds(m, groups, stride=part_rows)
        parts = []
        for p in range(evens):
            first = 2 * p * length // 128
            tiles = [rows_ref[first + t, here, :] for t in range(head // 128 + 1)]
            parts.append(jnp.concatenate(tiles, axis=1)[:, :length])
        even = jnp.concatenate(parts, axis=0).astype(BF16)
        result = dot(even, place_even, (0, 0))
        parts = []
        for p in range(odds):
            first = (2 * p * length + head) // 128
            tiles = [rows_ref[first + t, here, :] for t in range(head // 128 + 1)]
            parts.append(jnp.concatenate(tiles, axis=1))
        odd = jnp.concatenate(parts, axis=0).astype(BF16)
        result = result + dot(odd, place_odd, (0, 0))[tail:]
        out_ref[m] = jnp.where(new, result, x_ref[m].astype(F32)).astype(BF16)


def split(x):
    high = x.astype(BF16)
    return high, (x - high.astype(F32)).astype(BF16)


def left_of(x):
    high, low = split(x)
    return jnp.concatenate([high, low, high, low], axis=1)


def right_of(x):
    high, low = split(x)
    return jnp.concatenate([high, high, low, low], axis=0)


def total(x):
    return jnp.sum(jnp.sum(x, axis=0, keepdims=True), axis=1, keepdims=True)


def transform_kernel(
    count_ref, dep_ref, inn_ref, prec_ref, out_ref, scaled_ref, h_ref, right_ref, rest_ref, inner_ref
):
    slots, members = out_ref.shape[0], out_ref.shape[1]
    obs = dep_ref.shape[1]
    rank = members - 1.0
    eye = (iota((members, members), 0) == iota((members, members), 1)).astype(F32)
    on_diagonal = iota((obs, obs), 0) == iota((obs, obs), 1)
    eye_obs = on_diagonal.astype(F32)
    f, z, norm_inv, signal = [], [], [], []
    for i in range(slots):
        weight = jnp.where(iota((1, obs), 1) < count_ref[i], jnp.sqrt(prec_ref[i : i + 1, :]), 0.0)
        column = jnp.sum(jnp.where(on_diagonal, weight, 0.0), axis=1, keepdims=True)
        scaled = (dep_ref[i].astype(F32) * column).astype(BF16)
        scaled_ref[i] = scaled
        signal.append((weight * inn_ref[i : i + 1, :]).astype(BF16).astype(F32))
        outer = dot(scaled, scaled, (1, 1))
        squares = total(outer * outer) + (2.0 * rank) * total(outer * eye_obs)
        norm_inv.append(1.0 / jnp.sqrt(squares + members * rank * rank))
        f.append(1.5 - (0.5 * rank) * norm_inv[i])
        z.append(f[i])
        h_ref[i] = outer * norm_inv[i]
    for i in range(slots):
        h = h_ref[i]
        right = right_of(h)
        right_ref[i] = right
        second = 0.25 * h - f[i] * eye_obs
        third = (f[i] * second + (0.5 * f[i]) * h - (0.5 * f[i] * f[i]) * eye_obs) - 0.125 * dot(
            left_of(h), right, (1, 0)
        )
        rest_ref[i] = third - 1.5 * second
        inner_ref[i] = -0.5 * eye_obs
        f[i] = 1.5 - 1.5 * f[i] * f[i] + f[i] * f[i] * f[i]

    def step(_, carried):
        f, z = list(carried[:slots]), list(carried[slots:])
        moved = [left_of(dot(left_of(rest_ref[i]), right_ref[i], (1, 0))) for i in range(slots)]
        seconds = []
        for i in range(slots):
            rest, inner = rest_ref[i], inner_ref[i]
            both = dot(moved[i], right_of(jnp.concatenate([inner, rest], axis=1)), (1, 0))
            inner_ref[i] = f[i] * inner + z[i] * rest + both[:, :obs]
            seconds.append((2.0 * f[i]) * rest + both[:, obs:])
            z[i] = f[i] * z[i]
        for i in range(slots):
            third = dot(moved[i], right_of(seconds[i]), (1, 0))
            third = third + f[i] * seconds[i] + (f[i] * f[i]) * rest_ref[i]
            rest_ref[i] = third - 1.5 * seconds[i]
            f[i] = 1.5 - 1.5 * f[i] * f[i] + f[i] * f[i] * f[i]
        return tuple(f) + tuple(z)

    carried = lax.fori_loop(0, ITERS - 2, step, tuple(f) + tuple(z))
    f, z = carried[:slots], carried[slots:]
    for i in range(slots):
        rest, inner = rest_ref[i], inner_ref[i]
        moved = left_of(dot(left_of(rest), right_ref[i], (1, 0)))
        inner_ref[i] = f[i] * inner + z[i] * rest + dot(moved, right_of(inner), (1, 0))
    for i in range(slots):
        inner, h, scaled = inner_ref[i], h_ref[i], scaled_ref[i]
        scale = f[i] * z[i]
        pull = signal[i]
        for _ in range(2):
            across = jnp.sum(inner * pull, axis=1, keepdims=True)
            pull = scale * pull + jnp.sum(h * across, axis=0, keepdims=True)
        pieces = []
        for _ in range(3):
            pieces.append(pull.astype(BF16).astype(F32))
            pull = pull - pieces[-1]
        pieces.append(jnp.zeros((5, obs), F32))
        rows = dot(jnp.concatenate(pieces, axis=0).astype(BF16), scaled, (1, 0))
        shift = jnp.sum(rows, axis=0, keepdims=True) * norm_inv[i]
        twice = jnp.concatenate([scaled, scaled], axis=0)
        spanned = dot(jnp.concatenate(split(inner), axis=1), twice, (1, 0))
        spanned = dot(twice, jnp.concatenate(split(spanned), axis=0), (0, 0))
        gain = jnp.sqrt(rank * norm_inv[i])
        out_ref[i] = (gain * (scale * eye + norm_inv[i] * spanned) + shift).astype(BF16)


def apply_kernel(y_ref, t_ref, out_ref, *, first, slots, length):
    members = y_ref.shape[0]
    head = (length // 128) * 128
    tail = length - head
    low = iota((members, 128), 1) < tail
    for p in range((slots + 1) // 2):
        base = 2 * p * length
        size = 2 * length if 2 * p + 1 < slots else length
        here = pl.ds(base, size)
        states = y_ref[:, here].astype(F32)
        average = jnp.sum(states, axis=0, keepdims=True) * (1.0 / members)
        spread = (states - average).astype(BF16)
        if size == length:
            update = dot(t_ref[first + 2 * p], spread, (1, 0))
        else:
            even = dot(t_ref[first + 2 * p], spread[:, : head + 128], (1, 0))
            odd = dot(t_ref[first + 2 * p + 1], spread[:, head:], (1, 0))
            update = jnp.concatenate(
                [even[:, :head], jnp.where(low, even[:, head:], odd[:, :128]), odd[:, 128:]], axis=1
            )
        out_ref[:, here] = (average + update).astype(BF16)


def exchange(blocks):
    return lax.all_to_all(blocks, "member", split_axis=0, concat_axis=0, tiled=True)


SMEM = pl.BlockSpec(memory_space=pltpu.SMEM)
VMEM = pl.BlockSpec(memory_space=pltpu.VMEM)
PARAMS = pltpu.CompilerParams(vmem_limit_bytes=48 * 2**20)


def lane_tiles(shape):
    return pltpu.VMEM((pl.cdiv(shape[1], 128), shape[0], 128), F32)


def pack(counts, states, chunks, groups, fewest):
    part_rows, length, width = states.shape
    rows = groups * part_rows
    scalar = jax.ShapeDtypeStruct((1,), jnp.int32)
    return pl.pallas_call(
        lambda *refs: pack_kernel(*refs, chunks=chunks, groups=groups, fewest=fewest),
        out_shape=[jax.ShapeDtypeStruct((rows, size * length), BF16) for _, size in chunks]
        + [scalar, scalar],
        in_specs=[SMEM, VMEM],
        out_specs=[VMEM] * len(chunks) + [SMEM, SMEM],
        scratch_shapes=[lane_tiles((rows, width // groups * length))],
        compiler_params=PARAMS,
        name="pack",
    )(counts, states)


def unpack(live, states, finished, slots, groups):
    part_rows, length, _ = states.shape
    return pl.pallas_call(
        lambda *refs: unpack_kernel(*refs, slots=slots, groups=groups),
        out_shape=jax.ShapeDtypeStruct(states.shape, BF16),
        in_specs=[SMEM, VMEM] + [VMEM] * len(finished),
        out_specs=VMEM,
        scratch_shapes=[lane_tiles((groups * part_rows, slots * length))],
        compiler_params=PARAMS,
        name="unpack",
    )(live, states, *finished)


def transforms(departures, innovations, precision, obs_count, slots):
    _, obs, members = departures.shape
    square = pltpu.VMEM((slots, obs, obs), F32)
    return pl.pallas_call(
        transform_kernel,
        out_shape=jax.ShapeDtypeStruct((slots, members, members), BF16),
        in_specs=[SMEM, VMEM, VMEM, VMEM],
        out_specs=VMEM,
        scratch_shapes=[
            pltpu.VMEM((slots, obs, members), BF16),
            square,
            pltpu.VMEM((slots, 4 * obs, obs), BF16),
            square,
            square,
        ],
        compiler_params=PARAMS,
        name="transform",
    )(obs_count, departures, innovations, precision)


def apply(states, transform, first, slots, length):
    return pl.pallas_call(
        lambda *refs: apply_kernel(*refs, first=first, slots=slots, length=length),
        out_shape=jax.ShapeDtypeStruct(states.shape, BF16),
        in_specs=[VMEM, VMEM],
        out_specs=VMEM,
        compiler_params=PARAMS,
        name="apply",
    )(states, transform)


def with_chunks(chunks, groups):
    def run(live, states, packed, departures, innovations, precision, obs_count):
        part_rows, length, _ = states.shape
        members = groups * part_rows

        def move(rows):
            blocks = rows.reshape(groups, part_rows, rows.shape[1])
            return exchange(blocks).reshape(members, rows.shape[1])

        arrived = [move(packed[chunk]) for chunk in chunks]
        slots = sum(size for _, size in chunks)
        transform = transforms(departures, innovations, precision, obs_count, slots)
        finished = [
            move(apply(columns, transform, start, size, length))
            for (start, size), columns in zip(chunks, arrived)
        ]
        return unpack(live, states, finished, slots, groups)

    return run


def on_device(ensemble, departures, innovations, precision, obs_count, tile_counts):
    groups = lax.axis_size("member")
    states = ensemble.transpose(0, 2, 1)
    plans = (((0, 2),), ((0, 3),), ((0, 4),))
    chunks = sorted({chunk for plan in plans for chunk in plan})
    *rows, index, live = pack(tile_counts, states, chunks, groups, 2)
    packed = dict(zip(chunks, rows))
    result = lax.switch(
        index[0],
        [with_chunks(plan, groups) for plan in plans],
        live,
        states,
        packed,
        departures,
        innovations,
        precision,
        obs_count,
    )
    return result.transpose(0, 2, 1)


def solution(mesh):
    placed = (
        P("member", "tile", None),
        P(("tile", "member"), None, None),
        P(("tile", "member"), None),
        P(("tile", "member"), None),
        P(("tile", "member")),
        P(),
    )
    return jax.shard_map(
        on_device, mesh=mesh, in_specs=placed, out_specs=P("member", "tile", None), check_vma=False
    )
```

```python
import jax
import jax.numpy as jnp
from jax import lax
from jax.experimental import pallas as pl
from jax.experimental.pallas import tpu as pltpu
from jax.sharding import PartitionSpec as P

ITERS = 6
IN_BLOCKS = 1
OUT_BLOCKS = 1
END_BLOCKS = 1
F32 = jnp.float32
BF16 = jnp.bfloat16


def iota(shape, axis):
    return lax.broadcasted_iota(jnp.int32, shape, axis)


def dot(a, b, dims):
    return lax.dot_general(a, b, ((dims[:1], dims[1:]), ((), ())), preferred_element_type=F32)


def pack_kernel(counts_ref, x_ref, *refs, plans, groups):
    out_refs, refs = refs[: len(plans)], refs[len(plans) :]
    mask_ref, index_ref, counts, x_buf, rows_ref, in_sems, out_sems, *out_bufs = refs
    part_rows, length, width = x_ref.shape
    capacity = width // groups
    head = (length // 128) * 128
    tail = length - head
    step = part_rows // IN_BLOCKS
    copies = []
    for k in range(IN_BLOCKS):
        here = pl.ds(k * step, step)
        copies.append(pltpu.make_async_copy(x_ref.at[here], x_buf.at[here], in_sems.at[k]))
    load = pltpu.make_async_copy(counts_ref, counts, in_sems.at[IN_BLOCKS])
    for copy in [load] + copies:
        copy.start()

    def pick(odd):
        shape = (capacity // 2 * groups, width)
        row = iota(shape, 0)
        slot = 2 * (row // groups) + odd
        return (iota(shape, 1) == (row % groups) * capacity + slot).astype(BF16)

    pick_even = pick(0)
    pick_odd = pick(1)
    low = iota((groups, 128), 1) < tail
    for m in range(part_rows):
        if m % step == 0:
            copies[m // step].wait()
        x = x_buf[m]
        even = dot(pick_even, jnp.concatenate([x, x[: 128 - tail]], axis=0), (1, 1))
        odd = dot(pick_odd, jnp.concatenate([x[head:], x], axis=0), (1, 1))
        here = pl.ds(m, groups, stride=part_rows)
        for p in range(capacity // 2):
            base = 2 * p * length // 128
            a = even[p * groups : (p + 1) * groups]
            b = odd[p * groups : (p + 1) * groups]
            joined = jnp.concatenate(
                [a[:, :head], jnp.where(low, a[:, head:], b[:, :128]), b[:, 128:]], axis=1
            )
            for t in range(2 * length // 128):
                rows_ref[base + t, here, :] = joined[:, 128 * t : 128 * (t + 1)]
    load.wait()
    live = counts[lax.axis_index("tile")] // groups
    index = jnp.clip(live, plans[0], plans[-1]) - plans[0]
    index_ref[0] = index
    mask_ref[...] = (iota(mask_ref.shape, 1) % capacity < live).astype(F32)
    block = groups * part_rows // OUT_BLOCKS
    for k, (slots, out_ref, out_buf) in enumerate(zip(plans, out_refs, out_bufs)):

        @pl.when(index == k)
        def _(slots=slots, out_ref=out_ref, out_buf=out_buf):
            sends = []
            for r in range(OUT_BLOCKS):
                rows = pl.ds(r * block, block)
                for t in range(pl.cdiv(slots * length, 128)):
                    end = min(128, slots * length - 128 * t)
                    out_buf[rows, pl.ds(128 * t, end)] = rows_ref[t, rows, :][:, :end].astype(BF16)
                sends.append(
                    pltpu.make_async_copy(
                        out_buf.at[rows], out_ref.at[rows], out_sems.at[k, r]
                    )
                )
                sends[r].start()
            for send in sends:
                send.wait()


def unpack_kernel(mask_ref, x_ref, y_ref, out_ref, rows_ref, out_buf, out_sems, *, groups):
    part_rows, length, width = out_ref.shape
    capacity = width // groups
    head = (length // 128) * 128
    tail = length - head
    new = jnp.broadcast_to(mask_ref[:1], (length, width)) > 0.0

    def place(count, odd):
        shape = (count * groups, width)
        row = iota(shape, 0)
        slot = 2 * (row // groups) + odd
        return (iota(shape, 1) == (row % groups) * capacity + slot).astype(BF16)

    pairs = capacity // 2
    place_even = place(pairs, 0)
    place_odd = place(pairs, 1)
    for t in range(rows_ref.shape[0]):
        end = min(128, y_ref.shape[1] - 128 * t)
        rows_ref[t, :, pl.ds(0, end)] = y_ref[:, pl.ds(128 * t, end)].astype(F32)
    copies = []
    step = part_rows // END_BLOCKS
    for m in range(part_rows):
        here = pl.ds(m, groups, stride=part_rows)
        evens, odds = [], []
        for p in range(pairs):
            first = 2 * p * length // 128
            tiles = [rows_ref[first + t, here, :] for t in range(2 * length // 128)]
            evens.append(jnp.concatenate(tiles[: head // 128 + 1], axis=1)[:, :length])
            odds.append(jnp.concatenate(tiles[head // 128 :], axis=1))
        even = jnp.concatenate(evens, axis=0).astype(BF16)
        odd = jnp.concatenate(odds, axis=0).astype(BF16)
        result = dot(even, place_even, (0, 0)) + dot(odd, place_odd, (0, 0))[tail:]
        out_buf[m] = jnp.where(new, result, x_ref[m].astype(F32)).astype(BF16)
        if (m + 1) % step == 0:
            done = pl.ds(m + 1 - step, step)
            copies.append(
                pltpu.make_async_copy(out_buf.at[done], out_ref.at[done], out_sems.at[m // step])
            )
            copies[-1].start()
    for copy in copies:
        copy.wait()


def split(x):
    high = x.astype(BF16)
    return high, (x - high.astype(F32)).astype(BF16)


def left_of(x):
    high, low = split(x)
    return jnp.concatenate([high, low, high, low], axis=1)


def right_of(x):
    high, low = split(x)
    return jnp.concatenate([high, high, low, low], axis=0)


def total(x):
    return jnp.sum(jnp.sum(x, axis=0, keepdims=True), axis=1, keepdims=True)


def transform_kernel(
    used_hbm, inn_hbm, prec_hbm, dep_hbm, out_ref, *refs
):
    used_ref, inn_ref, prec_ref, dep_ref, scaled_ref, h_ref, right_ref, rest_ref, inner_ref, sems = refs
    slots, members = out_ref.shape[0], out_ref.shape[1]
    obs = dep_ref.shape[1]
    loads = [
        pltpu.make_async_copy(source, target, sems.at[i])
        for i, (source, target) in enumerate(
            (
                (used_hbm, used_ref),
                (inn_hbm, inn_ref),
                (prec_hbm, prec_ref),
                (dep_hbm.at[pl.ds(0, slots)], dep_ref),
            )
        )
    ]
    for load in loads:
        load.start()
    for load in loads:
        load.wait()
    rank = members - 1.0
    eye = (iota((members, members), 0) == iota((members, members), 1)).astype(F32)
    on_diagonal = iota((obs, obs), 0) == iota((obs, obs), 1)
    eye_obs = on_diagonal.astype(F32)
    f, z, norm_inv, signal = [], [], [], []
    for i in range(slots):
        weight = jnp.where(iota((1, obs), 1) < used_ref[i], jnp.sqrt(prec_ref[i : i + 1, :]), 0.0)
        column = jnp.sum(jnp.where(on_diagonal, weight, 0.0), axis=1, keepdims=True)
        scaled = (dep_ref[i].astype(F32) * column).astype(BF16)
        scaled_ref[i] = scaled
        signal.append((weight * inn_ref[i : i + 1, :]).astype(BF16).astype(F32))
        outer = dot(scaled, scaled, (1, 1))
        squares = total(outer * outer) + (2.0 * rank) * total(outer * eye_obs)
        norm_inv.append(1.0 / jnp.sqrt(squares + members * rank * rank))
        f.append(1.5 - (0.5 * rank) * norm_inv[i])
        z.append(f[i])
        h_ref[i] = outer * norm_inv[i]
    for i in range(slots):
        h = h_ref[i]
        right = right_of(h)
        right_ref[i] = right
        second = 0.25 * h - f[i] * eye_obs
        third = (f[i] * second + (0.5 * f[i]) * h - (0.5 * f[i] * f[i]) * eye_obs) - 0.125 * dot(
            left_of(h), right, (1, 0)
        )
        rest_ref[i] = third - 1.5 * second
        inner_ref[i] = -0.5 * eye_obs
        f[i] = 1.5 - 1.5 * f[i] * f[i] + f[i] * f[i] * f[i]

    def step(_, carried):
        f, z = list(carried[:slots]), list(carried[slots:])
        moved = [left_of(dot(left_of(rest_ref[i]), right_ref[i], (1, 0))) for i in range(slots)]
        seconds = []
        for i in range(slots):
            rest, inner = rest_ref[i], inner_ref[i]
            both = dot(moved[i], right_of(jnp.concatenate([inner, rest], axis=1)), (1, 0))
            inner_ref[i] = f[i] * inner + z[i] * rest + both[:, :obs]
            seconds.append((2.0 * f[i]) * rest + both[:, obs:])
            z[i] = f[i] * z[i]
        for i in range(slots):
            third = dot(moved[i], right_of(seconds[i]), (1, 0))
            third = third + f[i] * seconds[i] + (f[i] * f[i]) * rest_ref[i]
            rest_ref[i] = third - 1.5 * seconds[i]
            f[i] = 1.5 - 1.5 * f[i] * f[i] + f[i] * f[i] * f[i]
        return tuple(f) + tuple(z)

    carried = lax.fori_loop(0, ITERS - 2, step, tuple(f) + tuple(z))
    f, z = carried[:slots], carried[slots:]
    for i in range(slots):
        rest, inner = rest_ref[i], inner_ref[i]
        moved = left_of(dot(left_of(rest), right_ref[i], (1, 0)))
        inner_ref[i] = f[i] * inner + z[i] * rest + dot(moved, right_of(inner), (1, 0))
    for i in range(slots):
        inner, h, scaled = inner_ref[i], h_ref[i], scaled_ref[i]
        scale = f[i] * z[i]
        pull = signal[i]
        for _ in range(2):
            across = jnp.sum(inner * pull, axis=1, keepdims=True)
            pull = scale * pull + jnp.sum(h * across, axis=0, keepdims=True)
        pieces = []
        for _ in range(3):
            pieces.append(pull.astype(BF16).astype(F32))
            pull = pull - pieces[-1]
        pieces.append(jnp.zeros((5, obs), F32))
        rows = dot(jnp.concatenate(pieces, axis=0).astype(BF16), scaled, (1, 0))
        shift = jnp.sum(rows, axis=0, keepdims=True) * norm_inv[i]
        twice = jnp.concatenate([scaled, scaled], axis=0)
        spanned = dot(jnp.concatenate(split(inner), axis=1), twice, (1, 0))
        spanned = dot(twice, jnp.concatenate(split(spanned), axis=0), (0, 0))
        gain = jnp.sqrt(rank * norm_inv[i])
        out_ref[i] = (gain * (scale * eye + norm_inv[i] * spanned) + shift).astype(BF16)


def apply_kernel(y_ref, t_ref, out_ref, *, slots, length):
    members = y_ref.shape[0]
    head = (length // 128) * 128
    tail = length - head
    low = iota((members, 128), 1) < tail
    for p in range((slots + 1) // 2):
        base = 2 * p * length
        size = 2 * length if 2 * p + 1 < slots else length
        here = pl.ds(base, size)
        states = y_ref[:, here].astype(F32)
        average = jnp.sum(states, axis=0, keepdims=True) * (1.0 / members)
        spread = (states - average).astype(BF16)
        if size == length:
            update = dot(t_ref[2 * p], spread, (1, 0))
        else:
            even = dot(t_ref[2 * p], spread[:, : head + 128], (1, 0))
            odd = dot(t_ref[2 * p + 1], spread[:, head:], (1, 0))
            update = jnp.concatenate(
                [even[:, :head], jnp.where(low, even[:, head:], odd[:, :128]), odd[:, 128:]], axis=1
            )
        out_ref[:, here] = (average + update).astype(BF16)


def exchange(blocks):
    return lax.all_to_all(blocks, "member", split_axis=0, concat_axis=0, tiled=True)


SMEM = pl.BlockSpec(memory_space=pltpu.SMEM)
VMEM = pl.BlockSpec(memory_space=pltpu.VMEM)
HBM = pl.BlockSpec(memory_space=pltpu.HBM)
PARAMS = pltpu.CompilerParams(vmem_limit_bytes=48 * 2**20)


def in_hbm(x):
    return pltpu.with_memory_space_constraint(x, pltpu.HBM)


def lane_tiles(shape):
    return pltpu.VMEM((pl.cdiv(shape[1], 128), shape[0], 128), F32)


def pack(counts, states, plans, groups):
    part_rows, length, width = states.shape
    rows = groups * part_rows
    return pl.pallas_call(
        lambda *refs: pack_kernel(*refs, plans=plans, groups=groups),
        out_shape=[jax.ShapeDtypeStruct((rows, slots * length), BF16) for slots in plans]
        + [jax.ShapeDtypeStruct((8, width), F32), jax.ShapeDtypeStruct((1,), jnp.int32)],
        in_specs=[HBM, HBM],
        out_specs=[HBM] * len(plans) + [VMEM, SMEM],
        scratch_shapes=[
            pltpu.SMEM(counts.shape, jnp.int32),
            pltpu.VMEM(states.shape, BF16),
            lane_tiles((rows, width // groups * length)),
            pltpu.SemaphoreType.DMA((IN_BLOCKS + 1,)),
            pltpu.SemaphoreType.DMA((len(plans), OUT_BLOCKS)),
        ]
        + [pltpu.VMEM((rows, slots * length), BF16) for slots in plans],
        compiler_params=PARAMS,
        name="pack",
    )(in_hbm(counts), in_hbm(states))


def unpack(mask, states, finished, groups):
    return pl.pallas_call(
        lambda *refs: unpack_kernel(*refs, groups=groups),
        out_shape=jax.ShapeDtypeStruct(states.shape, BF16),
        in_specs=[VMEM, VMEM, VMEM],
        out_specs=HBM,
        scratch_shapes=[
            lane_tiles(finished.shape),
            pltpu.VMEM(states.shape, BF16),
            pltpu.SemaphoreType.DMA((END_BLOCKS,)),
        ],
        compiler_params=PARAMS,
        name="unpack",
    )(mask, states, finished)


def transforms(used, innovations, precision, departures, slots):
    _, obs, members = departures.shape
    square = pltpu.VMEM((slots, obs, obs), F32)
    return pl.pallas_call(
        transform_kernel,
        out_shape=jax.ShapeDtypeStruct((slots, members, members), BF16),
        in_specs=[HBM] * 4,
        out_specs=VMEM,
        scratch_shapes=[
            pltpu.SMEM(used.shape, jnp.int32),
            pltpu.VMEM(innovations.shape, F32),
            pltpu.VMEM(precision.shape, F32),
            pltpu.VMEM((slots, obs, members), BF16),
            pltpu.VMEM((slots, obs, members), BF16),
            square,
            pltpu.VMEM((slots, 4 * obs, obs), BF16),
            square,
            square,
            pltpu.SemaphoreType.DMA((4,)),
        ],
        compiler_params=PARAMS,
        name="transform",
    )(*map(in_hbm, (used, innovations, precision, departures)))


def apply(states, transform, slots, length):
    return pl.pallas_call(
        lambda *refs: apply_kernel(*refs, slots=slots, length=length),
        out_shape=jax.ShapeDtypeStruct(states.shape, BF16),
        in_specs=[VMEM, VMEM],
        out_specs=VMEM,
        compiler_params=PARAMS,
        name="apply",
    )(states, transform)


def with_slots(k, plans, groups):
    def run(packed, used, innovations, precision, departures):
        slots = plans[k]
        members = departures.shape[2]
        part_rows = members // groups
        width = packed[k].shape[1]
        sent = packed[k].reshape(groups, part_rows, width)
        columns = exchange(sent).reshape(members, width)
        transform = transforms(used, innovations, precision, departures, slots)
        result = apply(columns, transform, slots, width // slots)
        home = exchange(result.reshape(groups, part_rows, width)).reshape(members, width)
        return jnp.pad(home, ((0, 0), (0, packed[-1].shape[1] - width)))

    return run


def on_device(ensemble, departures, innovations, precision, obs_count, tile_counts):
    groups = lax.axis_size("member")
    states = ensemble.transpose(0, 2, 1)
    plans = tuple(range(2, departures.shape[0] + 1))
    *packed, mask, index = pack(tile_counts, states, plans, groups)
    home = lax.switch(
        index[0],
        [with_slots(k, plans, groups) for k in range(len(plans))],
        packed,
        obs_count,
        innovations,
        precision,
        departures,
    )
    return unpack(mask, states, home, groups).transpose(0, 2, 1)


def solution(mesh):
    placed = (
        P("member", "tile", None),
        P(("tile", "member"), None, None),
        P(("tile", "member"), None),
        P(("tile", "member"), None),
        P(("tile", "member")),
        P(),
    )
    return jax.shard_map(
        on_device, mesh=mesh, in_specs=placed, out_specs=P("member", "tile", None), check_vma=False
    )
```

```python
import jax
import jax.numpy as jnp
from jax import lax
from jax.experimental import pallas as pl
from jax.experimental.pallas import tpu as pltpu
from jax.sharding import PartitionSpec as P

ITERS = 6
PACK_STEP = 8
UNPACK_STEP = 8
F32 = jnp.float32
BF16 = jnp.bfloat16


def iota(shape, axis):
    return lax.broadcasted_iota(jnp.int32, shape, axis)


def dot(a, b, dims):
    return lax.dot_general(a, b, ((dims[:1], dims[1:]), ((), ())), preferred_element_type=F32)


def in_steps(count, step, body):
    def several(k, carry):
        for i in range(step):
            body(k * step + i)
        return carry

    if step == count:
        several(0, 0)
    else:
        lax.fori_loop(0, count // step, several, 0)


def pack_kernel(counts_ref, x_ref, *refs, plans, groups):
    out_refs, refs = refs[: len(plans)], refs[len(plans) :]
    mask_ref, index_ref, counts, x_buf, rows_ref, out_buf, sems = refs
    part_rows, length, width = x_ref.shape
    capacity = width // groups
    head = (length // 128) * 128
    tail = length - head
    count_copy = pltpu.make_async_copy(counts_ref, counts, sems.at[0])
    state_copy = pltpu.make_async_copy(x_ref, x_buf, sems.at[1])
    count_copy.start()
    state_copy.start()

    def pick(odd):
        shape = (capacity // 2 * groups, width)
        row = iota(shape, 0)
        slot = 2 * (row // groups) + odd
        return (iota(shape, 1) == (row % groups) * capacity + slot).astype(BF16)

    pick_even = pick(0)
    pick_odd = pick(1)
    low = iota((groups, 128), 1) < tail
    state_copy.wait()

    def member(m):
        x = x_buf[m]
        even = dot(pick_even, jnp.concatenate([x, x[: 128 - tail]], axis=0), (1, 1))
        odd = dot(pick_odd, jnp.concatenate([x[head:], x], axis=0), (1, 1))
        here = pl.ds(m, groups, stride=part_rows)
        for p in range(capacity // 2):
            base = 2 * p * length // 128
            a = even[p * groups : (p + 1) * groups]
            b = odd[p * groups : (p + 1) * groups]
            joined = jnp.concatenate(
                [a[:, :head], jnp.where(low, a[:, head:], b[:, :128]), b[:, 128:]], axis=1
            )
            for t in range(2 * length // 128):
                rows_ref[base + t, here, :] = joined[:, 128 * t : 128 * (t + 1)]

    in_steps(part_rows, PACK_STEP, member)
    for t in range(rows_ref.shape[0]):
        out_buf[:, pl.ds(128 * t, 128)] = rows_ref[t].astype(BF16)
    count_copy.wait()
    live = counts[lax.axis_index("tile")] // groups
    index = jnp.clip(live, 0, capacity)
    index_ref[0] = index
    mask_ref[...] = (iota(mask_ref.shape, 1) % capacity < live).astype(F32)
    for slots, out_ref in zip(plans, out_refs):

        @pl.when(index == slots)
        def _(out_ref=out_ref):
            lanes = pl.ds(0, out_ref.shape[1])
            send = pltpu.make_async_copy(out_buf.at[:, lanes], out_ref, sems.at[2])
            send.start()
            send.wait()


def unpack_kernel(mask_ref, x_ref, y_ref, out_ref, rows_ref, out_buf, out_sem, *, groups):
    part_rows, length, width = out_ref.shape
    capacity = width // groups
    head = (length // 128) * 128
    tail = length - head
    new = jnp.broadcast_to(mask_ref[:1], (length, width)) > 0.0

    def place(count, odd):
        shape = (count * groups, width)
        row = iota(shape, 0)
        slot = 2 * (row // groups) + odd
        return (iota(shape, 1) == (row % groups) * capacity + slot).astype(BF16)

    pairs = capacity // 2
    place_even = place(pairs, 0)
    place_odd = place(pairs, 1)
    for t in range(rows_ref.shape[0]):
        end = min(128, y_ref.shape[1] - 128 * t)
        rows_ref[t, :, pl.ds(0, end)] = y_ref[:, pl.ds(128 * t, end)].astype(F32)

    def member(m):
        here = pl.ds(m, groups, stride=part_rows)
        evens, odds = [], []
        for p in range(pairs):
            first = 2 * p * length // 128
            tiles = [rows_ref[first + t, here, :] for t in range(2 * length // 128)]
            evens.append(jnp.concatenate(tiles[: head // 128 + 1], axis=1)[:, :length])
            odds.append(jnp.concatenate(tiles[head // 128 :], axis=1))
        even = jnp.concatenate(evens, axis=0).astype(BF16)
        odd = jnp.concatenate(odds, axis=0).astype(BF16)
        result = dot(even, place_even, (0, 0)) + dot(odd, place_odd, (0, 0))[tail:]
        out_buf[m] = jnp.where(new, result, x_ref[m].astype(F32)).astype(BF16)

    in_steps(part_rows, UNPACK_STEP, member)
    send = pltpu.make_async_copy(out_buf, out_ref, out_sem)
    send.start()
    send.wait()


def split(x):
    high = x.astype(BF16)
    return high, (x - high.astype(F32)).astype(BF16)


def left_of(x):
    high, low = split(x)
    return jnp.concatenate([high, low, high, low], axis=1)


def right_of(x):
    high, low = split(x)
    return jnp.concatenate([high, high, low, low], axis=0)


def total(x):
    return jnp.sum(jnp.sum(x, axis=0, keepdims=True), axis=1, keepdims=True)


def transform_kernel(
    used_hbm, inn_hbm, prec_hbm, dep_hbm, out_ref, *refs
):
    used_ref, inn_ref, prec_ref, dep_ref, scaled_ref, h_ref, right_ref, rest_ref, inner_ref, sems = refs
    slots, members = out_ref.shape[0], out_ref.shape[1]
    obs = dep_ref.shape[1]
    loads = [
        pltpu.make_async_copy(source, target, sems.at[i])
        for i, (source, target) in enumerate(
            (
                (used_hbm, used_ref),
                (inn_hbm, inn_ref),
                (prec_hbm, prec_ref),
                (dep_hbm.at[pl.ds(0, slots)], dep_ref),
            )
        )
    ]
    for load in loads:
        load.start()
    for load in loads:
        load.wait()
    rank = members - 1.0
    eye = (iota((members, members), 0) == iota((members, members), 1)).astype(F32)
    on_diagonal = iota((obs, obs), 0) == iota((obs, obs), 1)
    eye_obs = on_diagonal.astype(F32)
    f, z, norm_inv, signal = [], [], [], []
    for i in range(slots):
        weight = jnp.where(iota((1, obs), 1) < used_ref[i], jnp.sqrt(prec_ref[i : i + 1, :]), 0.0)
        column = jnp.sum(jnp.where(on_diagonal, weight, 0.0), axis=1, keepdims=True)
        scaled = (dep_ref[i].astype(F32) * column).astype(BF16)
        scaled_ref[i] = scaled
        signal.append((weight * inn_ref[i : i + 1, :]).astype(BF16).astype(F32))
        outer = dot(scaled, scaled, (1, 1))
        squares = total(outer * outer) + (2.0 * rank) * total(outer * eye_obs)
        norm_inv.append(1.0 / jnp.sqrt(squares + members * rank * rank))
        f.append(1.5 - (0.5 * rank) * norm_inv[i])
        z.append(f[i])
        h_ref[i] = outer * norm_inv[i]
    for i in range(slots):
        h = h_ref[i]
        right = right_of(h)
        right_ref[i] = right
        second = 0.25 * h - f[i] * eye_obs
        third = (f[i] * second + (0.5 * f[i]) * h - (0.5 * f[i] * f[i]) * eye_obs) - 0.125 * dot(
            left_of(h), right, (1, 0)
        )
        rest_ref[i] = third - 1.5 * second
        inner_ref[i] = -0.5 * eye_obs
        f[i] = 1.5 - 1.5 * f[i] * f[i] + f[i] * f[i] * f[i]

    def step(_, carried):
        f, z = list(carried[:slots]), list(carried[slots:])
        moved = [left_of(dot(left_of(rest_ref[i]), right_ref[i], (1, 0))) for i in range(slots)]
        seconds = []
        for i in range(slots):
            rest, inner = rest_ref[i], inner_ref[i]
            both = dot(moved[i], right_of(jnp.concatenate([inner, rest], axis=1)), (1, 0))
            inner_ref[i] = f[i] * inner + z[i] * rest + both[:, :obs]
            seconds.append((2.0 * f[i]) * rest + both[:, obs:])
            z[i] = f[i] * z[i]
        for i in range(slots):
            third = dot(moved[i], right_of(seconds[i]), (1, 0))
            third = third + f[i] * seconds[i] + (f[i] * f[i]) * rest_ref[i]
            rest_ref[i] = third - 1.5 * seconds[i]
            f[i] = 1.5 - 1.5 * f[i] * f[i] + f[i] * f[i] * f[i]
        return tuple(f) + tuple(z)

    carried = lax.fori_loop(0, ITERS - 2, step, tuple(f) + tuple(z))
    f, z = carried[:slots], carried[slots:]
    for i in range(slots):
        rest, inner = rest_ref[i], inner_ref[i]
        moved = left_of(dot(left_of(rest), right_ref[i], (1, 0)))
        inner_ref[i] = f[i] * inner + z[i] * rest + dot(moved, right_of(inner), (1, 0))
    for i in range(slots):
        inner, h, scaled = inner_ref[i], h_ref[i], scaled_ref[i]
        scale = f[i] * z[i]
        pull = signal[i]
        for _ in range(2):
            across = jnp.sum(inner * pull, axis=1, keepdims=True)
            pull = scale * pull + jnp.sum(h * across, axis=0, keepdims=True)
        pieces = []
        for _ in range(3):
            pieces.append(pull.astype(BF16).astype(F32))
            pull = pull - pieces[-1]
        pieces.append(jnp.zeros((5, obs), F32))
        rows = dot(jnp.concatenate(pieces, axis=0).astype(BF16), scaled, (1, 0))
        shift = jnp.sum(rows, axis=0, keepdims=True) * norm_inv[i]
        twice = jnp.concatenate([scaled, scaled], axis=0)
        spanned = dot(jnp.concatenate(split(inner), axis=1), twice, (1, 0))
        spanned = dot(twice, jnp.concatenate(split(spanned), axis=0), (0, 0))
        gain = jnp.sqrt(rank * norm_inv[i])
        out_ref[i] = (gain * (scale * eye + norm_inv[i] * spanned) + shift).astype(BF16)


def apply_kernel(y_ref, t_ref, out_ref, *, slots, length):
    members = y_ref.shape[0]
    head = (length // 128) * 128
    tail = length - head
    low = iota((members, 128), 1) < tail
    for p in range((slots + 1) // 2):
        base = 2 * p * length
        size = 2 * length if 2 * p + 1 < slots else head + 128
        here = pl.ds(base, size)
        states = y_ref[:, here].astype(F32)
        average = jnp.sum(states, axis=0, keepdims=True) * (1.0 / members)
        spread = (states - average).astype(BF16)
        if size != 2 * length:
            update = dot(t_ref[2 * p], spread, (1, 0))
        else:
            even = dot(t_ref[2 * p], spread[:, : head + 128], (1, 0))
            odd = dot(t_ref[2 * p + 1], spread[:, head:], (1, 0))
            update = jnp.concatenate(
                [even[:, :head], jnp.where(low, even[:, head:], odd[:, :128]), odd[:, 128:]], axis=1
            )
        out_ref[:, here] = (average + update).astype(BF16)


def exchange(blocks):
    return lax.all_to_all(blocks, "member", split_axis=0, concat_axis=0, tiled=True)


SMEM = pl.BlockSpec(memory_space=pltpu.SMEM)
VMEM = pl.BlockSpec(memory_space=pltpu.VMEM)
HBM = pl.BlockSpec(memory_space=pltpu.HBM)
PARAMS = pltpu.CompilerParams(vmem_limit_bytes=48 * 2**20)


def in_hbm(x):
    return pltpu.with_memory_space_constraint(x, pltpu.HBM)


def lanes_of(slots, length):
    return pl.cdiv(slots * length, 128) * 128


def lane_tiles(shape):
    return pltpu.VMEM((pl.cdiv(shape[1], 128), shape[0], 128), F32)


def pack(counts, states, plans, groups):
    part_rows, length, width = states.shape
    rows = groups * part_rows
    full = (rows, width // groups * length)
    return pl.pallas_call(
        lambda *refs: pack_kernel(*refs, plans=plans, groups=groups),
        out_shape=[jax.ShapeDtypeStruct((rows, lanes_of(slots, length)), BF16) for slots in plans]
        + [jax.ShapeDtypeStruct((8, width), F32), jax.ShapeDtypeStruct((1,), jnp.int32)],
        in_specs=[HBM, HBM],
        out_specs=[HBM] * len(plans) + [VMEM, SMEM],
        scratch_shapes=[
            pltpu.SMEM(counts.shape, jnp.int32),
            pltpu.VMEM(states.shape, BF16),
            lane_tiles(full),
            pltpu.VMEM(full, BF16),
            pltpu.SemaphoreType.DMA((3,)),
        ],
        compiler_params=PARAMS,
        name="pack",
    )(in_hbm(counts), in_hbm(states))


def unpack(mask, states, finished, groups):
    return pl.pallas_call(
        lambda *refs: unpack_kernel(*refs, groups=groups),
        out_shape=jax.ShapeDtypeStruct(states.shape, BF16),
        in_specs=[VMEM, VMEM, VMEM],
        out_specs=HBM,
        scratch_shapes=[
            lane_tiles(finished.shape),
            pltpu.VMEM(states.shape, BF16),
            pltpu.SemaphoreType.DMA(()),
        ],
        compiler_params=PARAMS,
        name="unpack",
    )(mask, states, finished)


def transforms(used, innovations, precision, departures, slots):
    _, obs, members = departures.shape
    square = pltpu.VMEM((slots, obs, obs), F32)
    return pl.pallas_call(
        transform_kernel,
        out_shape=jax.ShapeDtypeStruct((slots, members, members), BF16),
        in_specs=[HBM] * 4,
        out_specs=VMEM,
        scratch_shapes=[
            pltpu.SMEM(used.shape, jnp.int32),
            pltpu.VMEM(innovations.shape, F32),
            pltpu.VMEM(precision.shape, F32),
            pltpu.VMEM((slots, obs, members), BF16),
            pltpu.VMEM((slots, obs, members), BF16),
            square,
            pltpu.VMEM((slots, 4 * obs, obs), BF16),
            square,
            square,
            pltpu.SemaphoreType.DMA((4,)),
        ],
        compiler_params=PARAMS,
        name="transform",
    )(*map(in_hbm, (used, innovations, precision, departures)))


def apply(states, transform, slots, length):
    return pl.pallas_call(
        lambda *refs: apply_kernel(*refs, slots=slots, length=length),
        out_shape=jax.ShapeDtypeStruct(states.shape, BF16),
        in_specs=[VMEM, VMEM],
        out_specs=VMEM,
        compiler_params=PARAMS,
        name="apply",
    )(states, transform)


def with_slots(k, plans, groups):
    def run(packed, used, innovations, precision, departures):
        slots = plans[k]
        members = departures.shape[2]
        part_rows = members // groups
        width = packed[k].shape[1]
        length = packed[-1].shape[1] // plans[-1]
        sent = packed[k].reshape(groups, part_rows, width)
        columns = exchange(sent).reshape(members, width)
        transform = transforms(used, innovations, precision, departures, slots)
        result = apply(columns, transform, slots, length)
        home = exchange(result.reshape(groups, part_rows, width)).reshape(members, width)
        return jnp.pad(home, ((0, 0), (0, packed[-1].shape[1] - width)))

    return run


def idle(packed, *_):
    return jnp.zeros_like(packed[-1])


def on_device(ensemble, departures, innovations, precision, obs_count, tile_counts):
    groups = lax.axis_size("member")
    states = ensemble.transpose(0, 2, 1)
    plans = tuple(range(1, departures.shape[0] + 1))
    *packed, mask, index = pack(tile_counts, states, plans, groups)
    home = lax.switch(
        index[0],
        [idle] + [with_slots(k, plans, groups) for k in range(len(plans))],
        packed,
        obs_count,
        innovations,
        precision,
        departures,
    )
    return unpack(mask, states, home, groups).transpose(0, 2, 1)


def solution(mesh):
    placed = (
        P("member", "tile", None),
        P(("tile", "member"), None, None),
        P(("tile", "member"), None),
        P(("tile", "member"), None),
        P(("tile", "member")),
        P(),
    )
    return jax.shard_map(
        on_device, mesh=mesh, in_specs=placed, out_specs=P("member", "tile", None), check_vma=False
    )
```

```python
import jax
import jax.numpy as jnp
from jax import lax
from jax.experimental import pallas as pl
from jax.experimental.pallas import tpu as pltpu
from jax.sharding import PartitionSpec as P

ITERS = 6
PACK_STEP = 8
UNPACK_STEP = 8
F32 = jnp.float32
BF16 = jnp.bfloat16


def iota(shape, axis):
    return lax.broadcasted_iota(jnp.int32, shape, axis)


def dot(a, b, dims):
    return lax.dot_general(a, b, ((dims[:1], dims[1:]), ((), ())), preferred_element_type=F32)


def in_steps(count, step, body):
    def several(k, carry):
        for i in range(step):
            body(k * step + i)
        return carry

    if step == count:
        several(0, 0)
    else:
        lax.fori_loop(0, count // step, several, 0)


def pack_kernel(counts_ref, x_ref, *refs, plans, groups):
    out_refs, refs = refs[: len(plans)], refs[len(plans) :]
    mask_ref, index_ref, counts, x_buf, rows_ref, out_buf, sems = refs
    part_rows, length, width = x_ref.shape
    capacity = width // groups
    head = (length // 128) * 128
    tail = length - head
    count_copy = pltpu.make_async_copy(counts_ref, counts, sems.at[0])
    state_copy = pltpu.make_async_copy(x_ref, x_buf, sems.at[1])
    count_copy.start()
    state_copy.start()

    def pick(odd):
        shape = (capacity // 2 * groups, width)
        row = iota(shape, 0)
        slot = 2 * (row // groups) + odd
        return (iota(shape, 1) == (row % groups) * capacity + slot).astype(BF16)

    pick_even = pick(0)
    pick_odd = pick(1)
    low = iota((groups, 128), 1) < tail
    state_copy.wait()

    def member(m):
        x = x_buf[m]
        even = dot(pick_even, jnp.concatenate([x, x[: 128 - tail]], axis=0), (1, 1))
        odd = dot(pick_odd, jnp.concatenate([x[head:], x], axis=0), (1, 1))
        here = pl.ds(m, groups, stride=part_rows)
        for p in range(capacity // 2):
            base = 2 * p * length // 128
            a = even[p * groups : (p + 1) * groups]
            b = odd[p * groups : (p + 1) * groups]
            joined = jnp.concatenate(
                [a[:, :head], jnp.where(low, a[:, head:], b[:, :128]), b[:, 128:]], axis=1
            )
            for t in range(2 * length // 128):
                rows_ref[base + t, here, :] = joined[:, 128 * t : 128 * (t + 1)]

    in_steps(part_rows, PACK_STEP, member)
    for t in range(rows_ref.shape[0]):
        out_buf[:, pl.ds(128 * t, 128)] = rows_ref[t].astype(BF16)
    count_copy.wait()
    live = counts[lax.axis_index("tile")] // groups
    index = jnp.clip(live, 0, capacity)
    index_ref[...] = jnp.full(index_ref.shape, index, jnp.int32)
    mask_ref[...] = (iota(mask_ref.shape, 1) % capacity < live).astype(F32)
    for slots, out_ref in zip(plans, out_refs):

        @pl.when(index == slots)
        def _(out_ref=out_ref):
            lanes = pl.ds(0, out_ref.shape[1])
            send = pltpu.make_async_copy(out_buf.at[:, lanes], out_ref, sems.at[2])
            send.start()
            send.wait()


def unpack_kernel(mask_ref, x_ref, y_ref, out_ref, rows_ref, out_buf, out_sem, *, groups):
    part_rows, length, width = out_ref.shape
    capacity = width // groups
    head = (length // 128) * 128
    tail = length - head
    new = jnp.broadcast_to(mask_ref[:1], (length, width)) > 0.0

    def place(count, odd):
        shape = (count * groups, width)
        row = iota(shape, 0)
        slot = 2 * (row // groups) + odd
        return (iota(shape, 1) == (row % groups) * capacity + slot).astype(BF16)

    pairs = capacity // 2
    place_even = place(pairs, 0)
    place_odd = place(pairs, 1)
    for t in range(rows_ref.shape[0]):
        end = min(128, y_ref.shape[1] - 128 * t)
        rows_ref[t, :, pl.ds(0, end)] = y_ref[:, pl.ds(128 * t, end)].astype(F32)

    def member(m):
        here = pl.ds(m, groups, stride=part_rows)
        evens, odds = [], []
        for p in range(pairs):
            first = 2 * p * length // 128
            tiles = [rows_ref[first + t, here, :] for t in range(2 * length // 128)]
            evens.append(jnp.concatenate(tiles[: head // 128 + 1], axis=1)[:, :length])
            odds.append(jnp.concatenate(tiles[head // 128 :], axis=1))
        even = jnp.concatenate(evens, axis=0).astype(BF16)
        odd = jnp.concatenate(odds, axis=0).astype(BF16)
        result = dot(even, place_even, (0, 0)) + dot(odd, place_odd, (0, 0))[tail:]
        out_buf[m] = jnp.where(new, result, x_ref[m].astype(F32)).astype(BF16)

    in_steps(part_rows, UNPACK_STEP, member)
    send = pltpu.make_async_copy(out_buf, out_ref, out_sem)
    send.start()
    send.wait()


def split(x):
    high = x.astype(BF16)
    return high, (x - high.astype(F32)).astype(BF16)


def left_of(x):
    high, low = split(x)
    return jnp.concatenate([high, low, high, low], axis=1)


def right_of(x):
    high, low = split(x)
    return jnp.concatenate([high, high, low, low], axis=0)


def total(x):
    return jnp.sum(jnp.sum(x, axis=0, keepdims=True), axis=1, keepdims=True)


def transform_kernel(
    used_hbm, inn_hbm, prec_hbm, dep_hbm, out_ref, *refs
):
    used_ref, inn_ref, prec_ref, dep_ref, scaled_ref, h_ref, right_ref, rest_ref, inner_ref, sems = refs
    slots, members = out_ref.shape[0], out_ref.shape[1]
    obs = dep_ref.shape[1]
    loads = [
        pltpu.make_async_copy(source, target, sems.at[i])
        for i, (source, target) in enumerate(
            (
                (used_hbm, used_ref),
                (inn_hbm, inn_ref),
                (prec_hbm, prec_ref),
                (dep_hbm.at[pl.ds(0, slots)], dep_ref),
            )
        )
    ]
    for load in loads:
        load.start()
    for load in loads:
        load.wait()
    rank = members - 1.0
    eye = (iota((members, members), 0) == iota((members, members), 1)).astype(F32)
    on_diagonal = iota((obs, obs), 0) == iota((obs, obs), 1)
    eye_obs = on_diagonal.astype(F32)
    f, z, norm_inv, signal = [], [], [], []
    for i in range(slots):
        weight = jnp.where(iota((1, obs), 1) < used_ref[i], jnp.sqrt(prec_ref[i : i + 1, :]), 0.0)
        column = jnp.sum(jnp.where(on_diagonal, weight, 0.0), axis=1, keepdims=True)
        scaled = (dep_ref[i].astype(F32) * column).astype(BF16)
        scaled_ref[i] = scaled
        signal.append((weight * inn_ref[i : i + 1, :]).astype(BF16).astype(F32))
        outer = dot(scaled, scaled, (1, 1))
        squares = total(outer * outer) + (2.0 * rank) * total(outer * eye_obs)
        norm_inv.append(1.0 / jnp.sqrt(squares + members * rank * rank))
        f.append(1.5 - (0.5 * rank) * norm_inv[i])
        z.append(f[i])
        h_ref[i] = outer * norm_inv[i]
    for i in range(slots):
        h = h_ref[i]
        right = right_of(h)
        right_ref[i] = right
        second = 0.25 * h - f[i] * eye_obs
        third = (f[i] * second + (0.5 * f[i]) * h - (0.5 * f[i] * f[i]) * eye_obs) - 0.125 * dot(
            left_of(h), right, (1, 0)
        )
        rest_ref[i] = third - 1.5 * second
        inner_ref[i] = -0.5 * eye_obs
        f[i] = 1.5 - 1.5 * f[i] * f[i] + f[i] * f[i] * f[i]

    def step(_, carried):
        f, z = list(carried[:slots]), list(carried[slots:])
        moved = [left_of(dot(left_of(rest_ref[i]), right_ref[i], (1, 0))) for i in range(slots)]
        seconds = []
        for i in range(slots):
            rest, inner = rest_ref[i], inner_ref[i]
            both = dot(moved[i], right_of(jnp.concatenate([inner, rest], axis=1)), (1, 0))
            inner_ref[i] = f[i] * inner + z[i] * rest + both[:, :obs]
            seconds.append((2.0 * f[i]) * rest + both[:, obs:])
            z[i] = f[i] * z[i]
        for i in range(slots):
            third = dot(moved[i], right_of(seconds[i]), (1, 0))
            third = third + f[i] * seconds[i] + (f[i] * f[i]) * rest_ref[i]
            rest_ref[i] = third - 1.5 * seconds[i]
            f[i] = 1.5 - 1.5 * f[i] * f[i] + f[i] * f[i] * f[i]
        return tuple(f) + tuple(z)

    carried = lax.fori_loop(0, ITERS - 2, step, tuple(f) + tuple(z))
    f, z = carried[:slots], carried[slots:]
    for i in range(slots):
        rest, inner = rest_ref[i], inner_ref[i]
        moved = left_of(dot(left_of(rest), right_ref[i], (1, 0)))
        inner_ref[i] = f[i] * inner + z[i] * rest + dot(moved, right_of(inner), (1, 0))
    for i in range(slots):
        inner, h, scaled = inner_ref[i], h_ref[i], scaled_ref[i]
        scale = f[i] * z[i]
        pull = signal[i]
        for _ in range(2):
            across = jnp.sum(inner * pull, axis=1, keepdims=True)
            pull = scale * pull + jnp.sum(h * across, axis=0, keepdims=True)
        pieces = []
        for _ in range(3):
            pieces.append(pull.astype(BF16).astype(F32))
            pull = pull - pieces[-1]
        pieces.append(jnp.zeros((5, obs), F32))
        rows = dot(jnp.concatenate(pieces, axis=0).astype(BF16), scaled, (1, 0))
        shift = jnp.sum(rows, axis=0, keepdims=True) * norm_inv[i]
        twice = jnp.concatenate([scaled, scaled], axis=0)
        spanned = dot(jnp.concatenate(split(inner), axis=1), twice, (1, 0))
        spanned = dot(twice, jnp.concatenate(split(spanned), axis=0), (0, 0))
        gain = jnp.sqrt(rank * norm_inv[i])
        out_ref[i] = (gain * (scale * eye + norm_inv[i] * spanned) + shift).astype(BF16)


def apply_kernel(y_ref, t_ref, out_ref, *, slots, length):
    members = y_ref.shape[0]
    head = (length // 128) * 128
    tail = length - head
    low = iota((members, 128), 1) < tail
    for p in range((slots + 1) // 2):
        base = 2 * p * length
        size = 2 * length if 2 * p + 1 < slots else head + 128
        here = pl.ds(base, size)
        states = y_ref[:, here].astype(F32)
        average = jnp.sum(states, axis=0, keepdims=True) * (1.0 / members)
        spread = (states - average).astype(BF16)
        if size != 2 * length:
            update = dot(t_ref[2 * p], spread, (1, 0))
        else:
            even = dot(t_ref[2 * p], spread[:, : head + 128], (1, 0))
            odd = dot(t_ref[2 * p + 1], spread[:, head:], (1, 0))
            update = jnp.concatenate(
                [even[:, :head], jnp.where(low, even[:, head:], odd[:, :128]), odd[:, 128:]], axis=1
            )
        out_ref[:, here] = (average + update).astype(BF16)


def exchange(blocks):
    return lax.all_to_all(blocks, "member", split_axis=0, concat_axis=0, tiled=True)


SMEM = pl.BlockSpec(memory_space=pltpu.SMEM)
VMEM = pl.BlockSpec(memory_space=pltpu.VMEM)
HBM = pl.BlockSpec(memory_space=pltpu.HBM)
PARAMS = pltpu.CompilerParams(vmem_limit_bytes=48 * 2**20)


def in_hbm(x):
    return pltpu.with_memory_space_constraint(x, pltpu.HBM)


def lanes_of(slots, length):
    return pl.cdiv(slots * length, 128) * 128


def lane_tiles(shape):
    return pltpu.VMEM((pl.cdiv(shape[1], 128), shape[0], 128), F32)


def pack(counts, states, plans, groups):
    part_rows, length, width = states.shape
    rows = groups * part_rows
    full = (rows, width // groups * length)
    return pl.pallas_call(
        lambda *refs: pack_kernel(*refs, plans=plans, groups=groups),
        out_shape=[jax.ShapeDtypeStruct((rows, lanes_of(slots, length)), BF16) for slots in plans]
        + [jax.ShapeDtypeStruct((8, width), F32), jax.ShapeDtypeStruct((1, 128), jnp.int32)],
        in_specs=[HBM, HBM],
        out_specs=[HBM] * len(plans) + [VMEM, VMEM],
        scratch_shapes=[
            pltpu.SMEM(counts.shape, jnp.int32),
            pltpu.VMEM(states.shape, BF16),
            lane_tiles(full),
            pltpu.VMEM(full, BF16),
            pltpu.SemaphoreType.DMA((3,)),
        ],
        compiler_params=PARAMS,
        name="pack",
    )(in_hbm(counts), in_hbm(states))


def unpack(mask, states, finished, groups):
    return pl.pallas_call(
        lambda *refs: unpack_kernel(*refs, groups=groups),
        out_shape=jax.ShapeDtypeStruct(states.shape, BF16),
        in_specs=[VMEM, VMEM, VMEM],
        out_specs=HBM,
        scratch_shapes=[
            lane_tiles(finished.shape),
            pltpu.VMEM(states.shape, BF16),
            pltpu.SemaphoreType.DMA(()),
        ],
        compiler_params=PARAMS,
        name="unpack",
    )(mask, states, finished)


def transforms(used, innovations, precision, departures, slots):
    _, obs, members = departures.shape
    square = pltpu.VMEM((slots, obs, obs), F32)
    return pl.pallas_call(
        transform_kernel,
        out_shape=jax.ShapeDtypeStruct((slots, members, members), BF16),
        in_specs=[HBM] * 4,
        out_specs=VMEM,
        scratch_shapes=[
            pltpu.SMEM(used.shape, jnp.int32),
            pltpu.VMEM(innovations.shape, F32),
            pltpu.VMEM(precision.shape, F32),
            pltpu.VMEM((slots, obs, members), BF16),
            pltpu.VMEM((slots, obs, members), BF16),
            square,
            pltpu.VMEM((slots, 4 * obs, obs), BF16),
            square,
            square,
            pltpu.SemaphoreType.DMA((4,)),
        ],
        compiler_params=PARAMS,
        name="transform",
    )(*map(in_hbm, (used, innovations, precision, departures)))


def apply(states, transform, slots, length):
    return pl.pallas_call(
        lambda *refs: apply_kernel(*refs, slots=slots, length=length),
        out_shape=jax.ShapeDtypeStruct(states.shape, BF16),
        in_specs=[VMEM, VMEM],
        out_specs=VMEM,
        compiler_params=PARAMS,
        name="apply",
    )(states, transform)


def with_slots(k, plans, groups):
    def run(packed, used, innovations, precision, departures):
        slots = plans[k]
        members = departures.shape[2]
        part_rows = members // groups
        width = packed[k].shape[1]
        length = packed[-1].shape[1] // plans[-1]
        sent = packed[k].reshape(groups, part_rows, width)
        columns = exchange(sent).reshape(members, width)
        transform = transforms(used, innovations, precision, departures, slots)
        result = apply(columns, transform, slots, length)
        home = exchange(result.reshape(groups, part_rows, width)).reshape(members, width)
        return jnp.pad(home, ((0, 0), (0, packed[-1].shape[1] - width)))

    return run


def idle(packed, *_):
    return jnp.zeros_like(packed[-1])


def on_device(ensemble, departures, innovations, precision, obs_count, tile_counts):
    groups = lax.axis_size("member")
    states = ensemble.transpose(0, 2, 1)
    plans = tuple(range(1, departures.shape[0] + 1))
    *packed, mask, index = pack(tile_counts, states, plans, groups)
    home = lax.switch(
        index[0, 0],
        [idle] + [with_slots(k, plans, groups) for k in range(len(plans))],
        packed,
        obs_count,
        innovations,
        precision,
        departures,
    )
    return unpack(mask, states, home, groups).transpose(0, 2, 1)


def solution(mesh):
    placed = (
        P("member", "tile", None),
        P(("tile", "member"), None, None),
        P(("tile", "member"), None),
        P(("tile", "member"), None),
        P(("tile", "member")),
        P(),
    )
    return jax.shard_map(
        on_device, mesh=mesh, in_specs=placed, out_specs=P("member", "tile", None), check_vma=False
    )
```
